8 devices in a mesh: dp: 1 (over z), ep: 8 (over x, y, core).
Axes of the slice: x: 2, y: 2, z: 1, core: 2. Of those that a mesh axis runs over, the one named last changes fastest.
Arguments:
- x: bfloat16 [1, 8, 384, 2048], P('dp', 'ep')
- expert: int32 [1, 8, 384, 6], P('dp', 'ep')
- slot: int32 [1, 8, 384, 6], P('dp', 'ep')
- gate: float32 [1, 8, 384, 6], P('dp', 'ep')
- w_gate: bfloat16 [64, 2048, 1408], P('ep')
- w_up: bfloat16 [64, 2048, 1408], P('ep')
- w_down: bfloat16 [64, 1408, 2048], P('ep')
- s_gate: bfloat16 [2048, 2816], replicated
- s_up: bfloat16 [2048, 2816], replicated
- s_down: bfloat16 [2816, 2048], replicated
Outputs:
- y: bfloat16 [1, 8, 384, 2048], P('dp', 'ep')
All inputs are finite; a program needn't handle non-finite values.
Results may differ from the reference program's by a relative error of at most 0.009.
Values are sent between devices in bfloat16 or wider.
A program may use at most 2 GiB of HBM per device.

```python
import jax
import jax.numpy as jnp

MEMBERS = 8
TOKENS = 384
D = 2048
FF = 1408
TOP = 6
EXPERTS = 64
SHARED_FF = 2816
SLOTS = 5 * TOKENS * TOP // (4 * EXPERTS)


def setup_inputs(seed: int = 0, part: int = 0) -> dict:
    own, k1, k2, k3, k4, k5, k6 = jax.random.split(jax.random.key(seed), 7)
    kx, ke, kl, kg = jax.random.split(jax.random.fold_in(own, part), 4)
    devices = (1, MEMBERS)
    place = jax.random.permutation(kl, jnp.arange(EXPERTS, dtype=jnp.uint32))
    slow = ((EXPERTS + (9 * place) % EXPERTS) << ((9 * place) // EXPERTS)) // EXPERTS
    wait = (jax.random.bits(ke, (*devices, TOKENS, EXPERTS), jnp.uint32) >> 10) * slow
    expert = jnp.argsort(wait, axis=-1)[..., :TOP].astype(jnp.int32)
    chosen = jax.nn.one_hot(expert, EXPERTS, dtype=jnp.int32)
    in_line = jnp.cumsum(chosen.reshape(*devices, TOKENS * TOP, EXPERTS), axis=2) - 1
    slot = jnp.sum(in_line.reshape(chosen.shape) * chosen, axis=-1)

    def one(key, rows, columns):
        return (jax.random.normal(key, (rows, columns), jnp.float32) * rows**-0.5).astype(jnp.bfloat16)

    def weights(key, rows, columns):
        return jax.lax.map(lambda k: one(k, rows, columns), jax.random.split(key, EXPERTS))

    return {
        "x": jax.random.normal(kx, (*devices, TOKENS, D), jnp.float32).astype(jnp.bfloat16),
        "expert": expert,
        "slot": slot,
        "gate": jax.nn.softmax(jax.random.normal(kg, expert.shape, jnp.float32)),
        "w_gate": weights(k1, D, FF),
        "w_up": weights(k2, D, FF),
        "w_down": weights(k3, FF, D),
        "s_gate": one(k4, D, SHARED_FF),
        "s_up": one(k5, D, SHARED_FF),
        "s_down": one(k6, SHARED_FF, D),
    }


def einsum(form, a, b):
    return jnp.einsum(form, a.astype(jnp.float32), b.astype(jnp.float32))


def for_all(x, s_gate, s_up, s_down):
    h = jax.nn.silu(einsum("...d,df->...f", x, s_gate)) * einsum("...d,df->...f", x, s_up)
    return einsum("...f,fd->...d", h.astype(jnp.bfloat16), s_down)


def reference(x, expert, slot, gate, w_gate, w_up, w_down, s_gate, s_up, s_down):
    to_expert = jax.nn.one_hot(expert, EXPERTS, dtype=jnp.bfloat16)
    to_slot = jax.nn.one_hot(slot, SLOTS, dtype=jnp.bfloat16)
    weighted = to_expert * gate[..., None].astype(jnp.bfloat16)
    dispatch = einsum("abtke,abtkc->abtec", to_expert, to_slot).astype(jnp.bfloat16)
    combine = einsum("abtke,abtkc->abtec", weighted, to_slot).astype(jnp.bfloat16)
    z = einsum("abtec,abtd->aebcd", dispatch, x).astype(jnp.bfloat16)
    h = jax.nn.silu(einsum("aebcd,edf->aebcf", z, w_gate))
    h = (h * einsum("aebcd,edf->aebcf", z, w_up)).astype(jnp.bfloat16)
    out = einsum("aebcf,efd->aebcd", h, w_down).astype(jnp.bfloat16)
    y = einsum("abtec,aebcd->abtd", combine, out)
    return (y + for_all(x, s_gate, s_up, s_down)).astype(jnp.bfloat16)
```

```python
import jax
import jax.numpy as jnp
from jax import lax
from jax.sharding import PartitionSpec as P


def dot(form, a, b):
    return jnp.einsum(form, a, b, preferred_element_type=jnp.float32)


def solution(mesh):
    members = mesh.shape["ep"]

    def body(x, expert, slot, gate, w_gate, w_up, w_down, s_gate, s_up, s_down):
        tokens, top = expert.shape[2:]
        own = w_gate.shape[0]
        slots = 5 * tokens * top // (4 * own * members)
        me = lax.axis_index("ep")
        x, expert, slot, gate = x[0, 0], expert[0, 0], slot[0, 0], gate[0, 0]
        place = jnp.where(slot < slots, expert * slots + slot, -1)
        xs = lax.all_gather(x, "ep")
        places = lax.all_gather(place, "ep")
        gates = lax.all_gather(gate, "ep").astype(jnp.bfloat16)
        rows = jnp.arange(own * slots, dtype=jnp.int32) + me * (own * slots)
        hit = places[..., None] == rows
        dispatch = jnp.any(hit, axis=2).astype(jnp.bfloat16)
        combine = jnp.sum(jnp.where(hit, gates[..., None], 0), axis=2).astype(jnp.bfloat16)
        z = dot("atc,atd->acd", dispatch, xs).astype(jnp.bfloat16)
        z = z.reshape(members, own, slots, -1)
        h = jax.nn.silu(dot("aecd,edf->eacf", z, w_gate)) * dot("aecd,edf->eacf", z, w_up)
        out = dot("eacf,efd->aecd", h.astype(jnp.bfloat16), w_down).astype(jnp.bfloat16)
        out = out.reshape(members, own * slots, -1)
        terms = dot("atc,acd->atd", combine, out).astype(jnp.bfloat16)
        y = lax.psum_scatter(terms, "ep", scatter_dimension=0)
        hs = jax.nn.silu(dot("td,df->tf", x, s_gate)) * dot("td,df->tf", x, s_up)
        y = y.astype(jnp.float32) + dot("tf,fd->td", hs.astype(jnp.bfloat16), s_down)
        return y.astype(jnp.bfloat16)[None, None]

    tok, exp, rep = P("dp", "ep"), P("ep"), P()
    return jax.shard_map(
        body,
        mesh=mesh,
        in_specs=(tok,) * 4 + (exp,) * 3 + (rep,) * 3,
        out_specs=tok,
        check_vma=False,
    )
```

```python
import functools

import jax
import jax.numpy as jnp
from jax import lax
from jax.experimental import pallas as pl
from jax.experimental.pallas import tpu as pltpu
from jax.sharding import PartitionSpec as P

MESH = pl.DeviceIdType.MESH
F32, BF16 = jnp.float32, jnp.bfloat16
VMEM_BYTES = 67043328
PAD = 48
OWN, NEAR, FAR, RELAY, LAST, PARTNER = (0, 1, 2), (0, 1), (3, 4), (3, 4, 5, 6), (7,), (2, 5, 6, 7)


def neighbours():
    me = lax.axis_index("ep")
    core, y, x = lax.rem(me, 2), lax.rem(me // 2, 2), me // 4
    return me, me + 4 - 8 * x, me + 2 - 4 * y, me + 1 - 2 * core


def greet(devices):
    barrier = pltpu.get_barrier_semaphore()
    for device in devices:
        pl.semaphore_signal(barrier, inc=1, device_id={"ep": device}, device_id_type=MESH)
    pl.semaphore_wait(barrier, len(devices))


def dot(a, b):
    return jnp.dot(a, b, preferred_element_type=F32)


def spread(width):
    return [(n, min(n + 256, width)) for n in range(0, width, 256)]


def first_kernel(
    dims, x_hbm, meta_hbm, wg, wu, sg, su, h_out, hs_out, ct_out,
    xg, meta, acc, wbuf, z, pm, stage, ctst, xsem, wsem, osem, csem, send, recv,
):
    pieces, width, tokens, ff, own, ring = dims
    me, xn, yn, pn = neighbours()
    half = tokens // 2
    shared_steps = 2 * pieces
    total = shared_steps + pieces * own

    def copies(ref, piece, rows, kinds):
        mid = rows // 2
        low, high = pl.ds(0, mid), pl.ds(mid, mid)
        plan = (
            (ref(0), ref(1), xn), (ref(0), ref(2), yn), (ref(0), ref(4), pn),
            (ref(1).at[low], ref(3).at[low], yn), (ref(2).at[high], ref(3).at[high], xn),
            (ref(1), ref(5), pn), (ref(2), ref(6), pn), (ref(3), ref(7), pn),
        )
        return [
            pltpu.make_async_remote_copy(
                src_ref=src, dst_ref=dst, send_sem=send.at[piece, kind], recv_sem=recv.at[piece, kind],
                device_id={"ep": device}, device_id_type=MESH,
            )
            for kind, (src, dst, device) in enumerate(plan) if kind in kinds
        ]

    def of_x(c, kinds):
        return copies(lambda q: xg.at[c, q], c, tokens, kinds)

    def of_meta(kinds):
        return copies(lambda q: meta.at[q], pieces, 16, kinds)

    def start(group):
        for copy in group:
            copy.start()

    def await_recv(group):
        for copy in group:
            copy.wait_recv()

    def load_x(c):
        return pltpu.make_async_copy(x_hbm.at[:, pl.ds(c * width, width)], xg.at[c, 0], xsem.at[c])

    load_meta = pltpu.make_async_copy(meta_hbm, meta.at[0], xsem.at[pieces])

    def w_copy(src, slot, part):
        return pltpu.make_async_copy(src, wbuf.at[slot, :, pl.ds(part * ff, ff)], wsem.at[slot, part])

    def fetch(g):
        slot = lax.rem(g, ring)

        @pl.when(g < shared_steps)
        def _():
            rows = pl.ds(pl.multiple_of(g // 2 * width, width), width)
            for which, src in enumerate((sg, su)):

                @pl.when(lax.rem(g, 2) == which)
                def _():
                    for part in range(2):
                        w_copy(src.at[rows, pl.ds(part * ff, ff)], slot, part).start()

        @pl.when(jnp.logical_and(g >= shared_steps, g < total))
        def _():
            at = g - shared_steps
            rows = pl.ds(pl.multiple_of(at // own * width, width), width)
            for part, src in enumerate((wg, wu)):
                w_copy(src.at[lax.rem(at, own), rows], slot, part).start()

    def await_w(slot):
        for part in range(2):
            w_copy(wg.at[0, pl.ds(0, width)], slot, part).wait()

    load_meta.start()
    for c in range(pieces):
        load_x(c).start()
    for g in range(ring - 1):
        fetch(jnp.int32(g))
    greet((xn, yn, pn))
    load_meta.wait()
    start(of_meta(OWN))
    for c in range(pieces):
        load_x(c).wait()
        if c < 2:
            start(of_x(c, OWN))

    def accumulate(e, c, lhs, slot):
        for n0, n1 in spread(2 * ff):
            old = jnp.where(c == 0, 0.0, acc[e, :, n0:n1])
            acc[e, :, n0:n1] = old + dot(lhs, wbuf[slot, :, n0:n1])

    def shared(g, _):
        fetch(g + ring - 1)
        slot = lax.rem(g, ring)
        await_w(slot)
        c = g // 2
        accumulate(lax.rem(g, 2), c, xg[c, 0], slot)

        @pl.when(g == 2)
        def _():
            await_recv(of_meta(NEAR))
            start(of_meta(RELAY))

        @pl.when(g == 6)
        def _():
            await_recv(of_meta(FAR))
            start(of_meta(LAST))

        @pl.when(g == 7)
        def _():
            relay(0)
            start(of_x(2, OWN))

        return 0

    def relay(c):
        await_recv(of_x(c, NEAR))
        start(of_x(c, RELAY))

    lax.fori_loop(0, shared_steps, shared, 0)

    def out_hs(part):
        return pltpu.make_async_copy(stage.at[part], hs_out.at[:, pl.ds(part * ff, ff)], osem.at[part])

    for part in range(2):
        for n0, n1 in spread(ff):
            at = slice(part * ff + n0, part * ff + n1)
            stage[part, :, n0:n1] = (jax.nn.silu(acc[0, :, at]) * acc[1, :, at]).astype(BF16)
        out_hs(part).start()

    await_recv(of_meta(PARTNER))
    base = (me * (own * PAD)).astype(F32)
    row = lax.broadcasted_iota(jnp.int32, (PAD, tokens), 0).astype(F32)

    def out_ct(q):
        return pltpu.make_async_copy(ctst.at[lax.rem(q, 2)], ct_out.at[q], csem.at[lax.rem(q, 2)])

    def one_hot(q, _):
        @pl.when(q >= 2)
        def _():
            out_ct(q - 2).wait()

        place, gate = meta[q, 0:8] - base, meta[q, 8:16]
        for e in range(own):
            p = jnp.zeros((PAD, tokens), F32)
            c = jnp.zeros((PAD, tokens), F32)
            for j in range(6):
                hit = (place[j : j + 1] - float(e * PAD)) == row
                p = jnp.where(hit, 1.0, p)
                c = jnp.where(hit, gate[j : j + 1], c)
            pm[q, e * PAD : (e + 1) * PAD] = p.astype(BF16)
            ctst[lax.rem(q, 2), e * PAD : (e + 1) * PAD] = c.astype(BF16)
        out_ct(q).start()
        return 0

    lax.fori_loop(0, 8, one_hot, 0)
    for q in (6, 7):
        out_ct(jnp.int32(q)).wait()
    for part in range(2):
        out_hs(part).wait()

    def gather(c):
        def place_rows(q):
            rows = dot(pm[q], xg[c, q]).astype(BF16)
            for e in range(own):
                z[e, q * PAD : (q + 1) * PAD] = rows[e * PAD : (e + 1) * PAD]

        await_recv(of_x(c, FAR))
        start(of_x(c, LAST))
        for q in range(4):
            place_rows(q)
        await_recv(of_x(c, PARTNER))
        for q in range(4, 8):
            place_rows(q)

    def piece(c, _):
        relay(c + 1)

        @pl.when(c + 3 < pieces)
        def _():
            start(of_x(c + 3, OWN))

        gather(c)

        def expert(e, _):
            g = shared_steps + c * own + e
            fetch(g + ring - 1)
            slot = lax.rem(g, ring)
            await_w(slot)
            accumulate(e, c, z[e], slot)
            return 0

        return lax.fori_loop(0, own, expert, 0)

    lax.fori_loop(0, pieces - 1, piece, 0)

    last = pieces - 1
    gather(last)

    def out_h(e):
        return pltpu.make_async_copy(stage.at[lax.rem(e, 2)], h_out.at[e], osem.at[lax.rem(e, 2)])

    def finish(e, _):
        g = shared_steps + last * own + e
        fetch(g + ring - 1)
        slot = lax.rem(g, ring)
        await_w(slot)

        @pl.when(e >= 2)
        def _():
            out_h(e - 2).wait()

        lhs = z[e]
        for n0, n1 in spread(ff):
            a = acc[e, :, n0:n1] + dot(lhs, wbuf[slot, :, n0:n1])
            b = acc[e, :, ff + n0 : ff + n1] + dot(lhs, wbuf[slot, :, ff + n0 : ff + n1])
            stage[lax.rem(e, 2), :, n0:n1] = (jax.nn.silu(a) * b).astype(BF16)
        out_h(e).start()
        return 0

    lax.fori_loop(0, own, finish, 0)
    for e in (own - 2, own - 1):
        out_h(jnp.int32(e)).wait()

    def drain(c, _):
        for copy in of_x(c, range(8)):
            copy.wait_send()
        return 0

    lax.fori_loop(0, pieces, drain, 0)
    for copy in of_meta(range(8)):
        copy.wait_send()


def second_kernel(
    dims, h_hbm, hs_hbm, ct_hbm, wd, sd, y_hbm,
    h, hs, ct, wbuf, sbuf, out, keep, dsend, drecv, s1, r1, s2, r2, yst,
    lsem, wsem, ssem, ysem, send, recv,
):
    tiles, width, tokens, own, ring = dims
    me, xn, yn, pn = neighbours()
    half = tokens // 2
    low, high = pl.ds(0, half), pl.ds(half, half)

    def remote(t, kind, src, dst, device):
        return pltpu.make_async_remote_copy(
            src_ref=src, dst_ref=dst, send_sem=send.at[t, kind], recv_sem=recv.at[t, kind],
            device_id={"ep": device}, device_id_type=MESH,
        )

    def to_partner(t):
        return remote(t, 0, dsend.at[t], drecv.at[t], pn)

    def phase_one(t):
        a, b = pl.ds(0, 2), pl.ds(2, 2)
        return (
            remote(t, 1, s1.at[t, a], r1.at[t, a], xn),
            remote(t, 2, s1.at[t, b], r1.at[t, b], yn),
        )

    def phase_two(t):
        return (
            remote(t, 3, s2.at[t, 0], r2.at[t, 0], yn),
            remote(t, 4, s2.at[t, 1], r2.at[t, 1], xn),
        )

    def columns(t):
        return pl.ds(pl.multiple_of(t * width, width), width)

    def w_copy(g):
        slot = lax.rem(g, ring)
        return pltpu.make_async_copy(wd.at[lax.rem(g, own), :, columns(g // own)], wbuf.at[slot], wsem.at[slot])

    def s_copy(t):
        slot = lax.rem(t, 2)
        return pltpu.make_async_copy(sd.at[:, columns(t)], sbuf.at[slot], ssem.at[slot])

    def h_copy(e):
        return pltpu.make_async_copy(h_hbm.at[e], h.at[e], lsem.at[e])

    def y_copy(t):
        slot = lax.rem(t, 2)
        return pltpu.make_async_copy(yst.at[slot], y_hbm.at[:, columns(t)], ysem.at[slot])

    load_ct = pltpu.make_async_copy(ct_hbm, ct, lsem.at[own])
    load_hs = pltpu.make_async_copy(hs_hbm, hs, lsem.at[own + 1])

    for e in range(own):
        h_copy(e).start()
        if e < ring - 1:
            w_copy(jnp.int32(e)).start()
    load_ct.start()
    load_hs.start()
    s_copy(jnp.int32(0)).start()
    greet((xn, yn, pn))

    def compute(t):
        @pl.when(t + 1 < tiles)
        def _():
            s_copy(t + 1).start()

        def expert(e, _):
            g = t * own + e

            @pl.when(g + ring - 1 < tiles * own)
            def _():
                w_copy(g + ring - 1).start()

            @pl.when(t == 0)
            def _():
                h_copy(e).wait()

            w_copy(g).wait()
            rows = dot(h[e], wbuf[lax.rem(g, ring)]).astype(BF16)
            at = pl.ds(pl.multiple_of(e * PAD, 16), PAD)
            for q in range(8):
                out[q, at] = rows[q * PAD : (q + 1) * PAD]
            return 0

        lax.fori_loop(0, own, expert, 0)

        @pl.when(t == 0)
        def _():
            load_ct.wait()
            load_hs.wait()

        def terms(q):
            return lax.dot_general(ct[q], out[q], (((0,), (0,)), ((), ())), preferred_element_type=F32)

        for q in range(4, 8):
            dsend[t, q - 4] = terms(q).astype(BF16)
        to_partner(t).start()
        s_copy(t).wait()
        keep[t, 0] = terms(0) + dot(hs[...], sbuf[lax.rem(t, 2)])
        for q in range(1, 4):
            keep[t, q] = terms(q)

    def stage_one(t):
        to_partner(t).wait_recv()

        def both(q, rows):
            return keep[t, q, rows] + drecv[t, q, rows].astype(F32)

        s1[t, 0] = both(1, low).astype(BF16)
        s1[t, 1] = both(3, low).astype(BF16)
        s1[t, 2] = both(2, high).astype(BF16)
        s1[t, 3] = both(3, high).astype(BF16)
        for copy in phase_one(t):
            copy.start()
        keep[t, 0] = keep[t, 0] + drecv[t, 0].astype(F32)
        keep[t, 1, high] = both(1, high)
        keep[t, 2, low] = both(2, low)

    def stage_two(t):
        for copy in phase_one(t):
            copy.wait_recv()
        s2[t, 0] = (keep[t, 2, low] + r1[t, 1].astype(F32)).astype(BF16)
        s2[t, 1] = (keep[t, 1, high] + r1[t, 3].astype(F32)).astype(BF16)
        for copy in phase_two(t):
            copy.start()
        keep[t, 0, low] = keep[t, 0, low] + r1[t, 0].astype(F32)
        keep[t, 0, high] = keep[t, 0, high] + r1[t, 2].astype(F32)

    def stage_three(t):
        for copy in phase_two(t):
            copy.wait_recv()

        @pl.when(t >= 2)
        def _():
            y_copy(t - 2).wait()

        slot = lax.rem(t, 2)
        yst[slot, low] = (keep[t, 0, low] + r2[t, 0].astype(F32)).astype(BF16)
        yst[slot, high] = (keep[t, 0, high] + r2[t, 1].astype(F32)).astype(BF16)
        y_copy(t).start()

    def tile(t, _):
        @pl.when(t < tiles)
        def _():
            compute(t)
            stage_one(t)

        @pl.when(jnp.logical_and(t >= 1, t <= tiles))
        def _():
            stage_two(t - 1)

        @pl.when(t >= 2)
        def _():
            stage_three(t - 2)

        return 0

    lax.fori_loop(0, tiles + 2, tile, 0)
    for t in (tiles - 2, tiles - 1):
        y_copy(jnp.int32(t)).wait()

    def drain(t, _):
        for copy in (to_partner(t), *phase_one(t), *phase_two(t)):
            copy.wait_send()
        return 0

    lax.fori_loop(0, tiles, drain, 0)


def solution(mesh):
    members = mesh.shape["ep"]

    def body(x, expert, slot, gate, w_gate, w_up, w_down, s_gate, s_up, s_down):
        tokens, top = expert.shape[2:]
        own, d, ff = w_gate.shape
        slots = 5 * tokens * top // (4 * own * members)
        x, expert, slot, gate = x[0, 0], expert[0, 0], slot[0, 0], gate[0, 0]
        place = jnp.where(slot < slots, expert * PAD + slot, -1).astype(F32)
        fill = ((0, 8 - top), (0, 0))
        meta = jnp.concatenate([jnp.pad(place.T, fill, constant_values=-1.0), jnp.pad(gate.T, fill)])

        hbm = pl.BlockSpec(memory_space=pl.ANY)
        dma = pltpu.SemaphoreType.DMA
        pieces, ring = 8, 4
        width = d // pieces
        rows = own * PAD
        h, hs, ct = pl.pallas_call(
            functools.partial(first_kernel, (pieces, width, tokens, ff, own, ring)),
            out_shape=(
                jax.ShapeDtypeStruct((own, rows, ff), BF16),
                jax.ShapeDtypeStruct((tokens, 2 * ff), BF16),
                jax.ShapeDtypeStruct((8, rows, tokens), BF16),
            ),
            in_specs=[hbm] * 6,
            out_specs=(hbm,) * 3,
            scratch_shapes=[
                pltpu.VMEM((pieces, 8, tokens, width), BF16),
                pltpu.VMEM((8, 16, tokens), F32),
                pltpu.VMEM((own, rows, 2 * ff), F32),
                pltpu.VMEM((ring, width, 2 * ff), BF16),
                pltpu.VMEM((own, rows, width), BF16),
                pltpu.VMEM((8, rows, tokens), BF16),
                pltpu.VMEM((2, rows, ff), BF16),
                pltpu.VMEM((2, rows, tokens), BF16),
                dma((pieces + 1,)),
                dma((ring, 2)),
                dma((2,)),
                dma((2,)),
                dma((pieces + 1, 8)),
                dma((pieces + 1, 8)),
            ],
            compiler_params=pltpu.CompilerParams(
                collective_id=0, has_side_effects=True, vmem_limit_bytes=VMEM_BYTES
            ),
            name="dispatch_up",
        )(x, meta, w_gate, w_up, s_gate, s_up)

        tiles, ring = 8, 6
        width = d // tiles
        y = pl.pallas_call(
            functools.partial(second_kernel, (tiles, width, tokens, own, ring)),
            out_shape=jax.ShapeDtypeStruct((tokens, d), BF16),
            in_specs=[hbm] * 5,
            out_specs=hbm,
            scratch_shapes=[
                pltpu.VMEM((own, rows, ff), BF16),
                pltpu.VMEM((tokens, 2 * ff), BF16),
                pltpu.VMEM((8, rows, tokens), BF16),
                pltpu.VMEM((ring, ff, width), BF16),
                pltpu.VMEM((2, 2 * ff, width), BF16),
                pltpu.VMEM((8, rows, width), BF16),
                pltpu.VMEM((tiles, 4, tokens, width), F32),
                pltpu.VMEM((tiles, 4, tokens, width), BF16),
                pltpu.VMEM((tiles, 4, tokens, width), BF16),
                pltpu.VMEM((tiles, 4, tokens // 2, width), BF16),
                pltpu.VMEM((tiles, 4, tokens // 2, width), BF16),
                pltpu.VMEM((tiles, 2, tokens // 2, width), BF16),
                pltpu.VMEM((tiles, 2, tokens // 2, width), BF16),
                pltpu.VMEM((2, tokens, width), BF16),
                dma((own + 2,)),
                dma((ring,)),
                dma((2,)),
                dma((2,)),
                dma((tiles, 5)),
                dma((tiles, 5)),
            ],
            compiler_params=pltpu.CompilerParams(
                collective_id=1, has_side_effects=True, vmem_limit_bytes=VMEM_BYTES
            ),
            name="down_combine",
        )(h, hs, ct, w_down, s_down)
        return y[None, None]

    tok, exp, rep = P("dp", "ep"), P("ep"), P()
    return jax.shard_map(
        body,
        mesh=mesh,
        in_specs=(tok,) * 4 + (exp,) * 3 + (rep,) * 3,
        out_specs=tok,
        check_vma=False,
    )
```

```python
import functools

import jax
import jax.numpy as jnp
from jax import lax
from jax.experimental import pallas as pl
from jax.experimental.pallas import tpu as pltpu
from jax.sharding import PartitionSpec as P

MESH = pl.DeviceIdType.MESH
F32, BF16 = jnp.float32, jnp.bfloat16
VMEM_BYTES = 67043328
GROUP = 4
PAD = 48
OWN, NEAR, FAR, RELAY, LAST, PARTNER = (0, 1, 2), (0, 1), (3, 4), (3, 4, 5, 6), (7,), (2, 5, 6, 7)


def neighbours():
    me = lax.axis_index("ep")
    core, y, x = lax.rem(me, 2), lax.rem(me // 2, 2), me // 4
    return me, me + 4 - 8 * x, me + 2 - 4 * y, me + 1 - 2 * core


def greet(devices):
    barrier = pltpu.get_barrier_semaphore()
    for device in devices:
        pl.semaphore_signal(barrier, inc=1, device_id={"ep": device}, device_id_type=MESH)
    pl.semaphore_wait(barrier, len(devices))


def dot(a, b):
    return jnp.dot(a, b, preferred_element_type=F32)


def spread(width):
    return [(n, min(n + 256, width)) for n in range(0, width, 256)]


def first_kernel(
    dims, x_hbm, meta_hbm, wg, wu, sg, su, h_out, hs_out, ct_out,
    xg, meta, acc, wbuf, z, pm, stage, ctst, xsem, wsem, osem, csem, send, recv,
):
    pieces, width, tokens, ff, own, ring = dims
    me, xn, yn, pn = neighbours()
    half = tokens // 2
    shared_steps = 2 * pieces
    total = shared_steps + pieces * own

    def copies(ref, piece, rows, kinds):
        mid = rows // 2
        low, high = pl.ds(0, mid), pl.ds(mid, mid)
        plan = (
            (ref(0), ref(1), xn), (ref(0), ref(2), yn), (ref(0), ref(4), pn),
            (ref(1).at[low], ref(3).at[low], yn), (ref(2).at[high], ref(3).at[high], xn),
            (ref(1), ref(5), pn), (ref(2), ref(6), pn), (ref(3), ref(7), pn),
        )
        return [
            pltpu.make_async_remote_copy(
                src_ref=src, dst_ref=dst, send_sem=send.at[piece, kind], recv_sem=recv.at[piece, kind],
                device_id={"ep": device}, device_id_type=MESH,
            )
            for kind, (src, dst, device) in enumerate(plan) if kind in kinds
        ]

    def of_x(c, kinds):
        return copies(lambda q: xg.at[c, q], c, tokens, kinds)

    def of_meta(kinds):
        return copies(lambda q: meta.at[q], pieces, 16, kinds)

    def start(group):
        for copy in group:
            copy.start()

    def await_recv(group):
        for copy in group:
            copy.wait_recv()

    def load_x(c):
        return pltpu.make_async_copy(x_hbm.at[:, pl.ds(c * width, width)], xg.at[c, 0], xsem.at[c])

    load_meta = pltpu.make_async_copy(meta_hbm, meta.at[0], xsem.at[pieces])

    def w_copy(src, slot, part):
        return pltpu.make_async_copy(src, wbuf.at[slot, :, pl.ds(part * ff, ff)], wsem.at[slot, part])

    def fetch(g):
        slot = lax.rem(g, ring)

        @pl.when(g < shared_steps)
        def _():
            rows = pl.ds(pl.multiple_of(g // 2 * width, width), width)
            for which, src in enumerate((sg, su)):

                @pl.when(lax.rem(g, 2) == which)
                def _():
                    for part in range(2):
                        w_copy(src.at[rows, pl.ds(part * ff, ff)], slot, part).start()

        @pl.when(jnp.logical_and(g >= shared_steps, g < total))
        def _():
            at = g - shared_steps
            rows = pl.ds(pl.multiple_of(at // own * width, width), width)
            for part, src in enumerate((wg, wu)):
                w_copy(src.at[lax.rem(at, own), rows], slot, part).start()

    def await_w(slot):
        for part in range(2):
            w_copy(wg.at[0, pl.ds(0, width)], slot, part).wait()

    load_meta.start()
    for c in range(pieces):
        load_x(c).start()
    for g in range(GROUP):
        fetch(jnp.int32(g))
    greet((xn, yn, pn))
    load_meta.wait()
    start(of_meta(OWN))
    for c in range(pieces):
        load_x(c).wait()
        if c < 2:
            start(of_x(c, OWN))

    def take(group):
        for i in range(GROUP):
            fetch((group + 1) * GROUP + i)
        slots = [lax.rem(group * GROUP + i, ring) for i in range(GROUP)]
        for slot in slots:
            await_w(slot)
        return slots

    def shared(p, _, new):
        slots = take(p)
        for which in range(2):
            for n0, n1 in spread(2 * ff):
                terms = sum(dot(xg[2 * p + i, 0], wbuf[slots[2 * i + which], :, n0:n1]) for i in range(2))
                acc[which, :, n0:n1] = terms if new else acc[which, :, n0:n1] + terms
        return 0

    def relay(c):
        await_recv(of_x(c, NEAR))
        start(of_x(c, RELAY))

    shared(0, 0, True)
    await_recv(of_meta(NEAR))
    start(of_meta(RELAY))

    def shared_rest(p, _):
        shared(p, 0, False)

        @pl.when(p == 1)
        def _():
            await_recv(of_meta(FAR))
            start(of_meta(LAST))

        @pl.when(p == 2)
        def _():
            relay(0)
            start(of_x(2, OWN))

        return 0

    lax.fori_loop(1, shared_steps // GROUP, shared_rest, 0)

    def out_hs(part):
        return pltpu.make_async_copy(stage.at[part], hs_out.at[:, pl.ds(part * ff, ff)], osem.at[part])

    for part in range(2):
        for n0, n1 in spread(ff):
            at = slice(part * ff + n0, part * ff + n1)
            stage[part, :, n0:n1] = (jax.nn.silu(acc[0, :, at]) * acc[1, :, at]).astype(BF16)
        out_hs(part).start()

    await_recv(of_meta(PARTNER))
    base = (me * (own * PAD)).astype(F32)
    row = lax.broadcasted_iota(jnp.int32, (PAD, tokens), 0).astype(F32)

    def out_ct(q):
        return pltpu.make_async_copy(ctst.at[lax.rem(q, 2)], ct_out.at[q], csem.at[lax.rem(q, 2)])

    def one_hot(q, _):
        @pl.when(q >= 2)
        def _():
            out_ct(q - 2).wait()

        place, gate = meta[q, 0:8] - base, meta[q, 8:16]
        for e in range(own):
            p = jnp.zeros((PAD, tokens), F32)
            c = jnp.zeros((PAD, tokens), F32)
            for j in range(6):
                hit = (place[j : j + 1] - float(e * PAD)) == row
                p = jnp.where(hit, 1.0, p)
                c = jnp.where(hit, gate[j : j + 1], c)
            pm[q, e * PAD : (e + 1) * PAD] = p.astype(BF16)
            ctst[lax.rem(q, 2), e * PAD : (e + 1) * PAD] = c.astype(BF16)
        out_ct(q).start()
        return 0

    lax.fori_loop(0, 8, one_hot, 0)
    for q in (6, 7):
        out_ct(jnp.int32(q)).wait()
    for part in range(2):
        out_hs(part).wait()

    def gather(c):
        def place_rows(q):
            rows = dot(pm[q], xg[c, q]).astype(BF16)
            for e in range(own):
                z[e, q * PAD : (q + 1) * PAD] = rows[e * PAD : (e + 1) * PAD]

        await_recv(of_x(c, FAR))
        start(of_x(c, LAST))
        for q in range(4):
            place_rows(q)
        await_recv(of_x(c, PARTNER))
        for q in range(4, 8):
            place_rows(q)

    def piece(c, _, new):
        relay(c + 1)

        @pl.when(c + 3 < pieces)
        def _():
            start(of_x(c + 3, OWN))

        gather(c)

        def experts(i, _):
            slots = take((shared_steps + c * own) // GROUP + i)
            for j, slot in enumerate(slots):
                e = i * GROUP + j
                lhs = z[e]
                for n0, n1 in spread(2 * ff):
                    term = dot(lhs, wbuf[slot, :, n0:n1])
                    acc[e, :, n0:n1] = term if new else acc[e, :, n0:n1] + term
            return 0

        return lax.fori_loop(0, own // GROUP, experts, 0)

    piece(jnp.int32(0), 0, True)
    lax.fori_loop(1, pieces - 1, functools.partial(piece, new=False), 0)

    last = pieces - 1
    gather(last)

    def out_h(e):
        return pltpu.make_async_copy(stage.at[lax.rem(e, 2)], h_out.at[e], osem.at[lax.rem(e, 2)])

    def finish(i, _):
        slots = take((shared_steps + last * own) // GROUP + i)
        for j, slot in enumerate(slots):
            e = i * GROUP + j
            if j >= 2:
                out_h(e - 2).wait()
            else:

                @pl.when(i > 0)
                def _():
                    out_h(e - 2).wait()

            lhs = z[e]
            for n0, n1 in spread(ff):
                a = acc[e, :, n0:n1] + dot(lhs, wbuf[slot, :, n0:n1])
                b = acc[e, :, ff + n0 : ff + n1] + dot(lhs, wbuf[slot, :, ff + n0 : ff + n1])
                stage[j % 2, :, n0:n1] = (jax.nn.silu(a) * b).astype(BF16)
            out_h(e).start()
        return 0

    lax.fori_loop(0, own // GROUP, finish, 0)
    for e in (own - 2, own - 1):
        out_h(jnp.int32(e)).wait()

    def drain(c, _):
        for copy in of_x(c, range(8)):
            copy.wait_send()
        return 0

    lax.fori_loop(0, pieces, drain, 0)
    for copy in of_meta(range(8)):
        copy.wait_send()


def second_kernel(
    dims, h_hbm, hs_hbm, ct_hbm, wd, sd, y_hbm,
    h, hs, ct, wbuf, sbuf, out, keep, dsend, drecv, s1, r1, s2, r2, yst,
    lsem, wsem, ssem, ysem, send, recv,
):
    tiles, width, tokens, own, ring = dims
    me, xn, yn, pn = neighbours()
    half = tokens // 2
    low, high = pl.ds(0, half), pl.ds(half, half)

    def remote(t, kind, src, dst, device):
        return pltpu.make_async_remote_copy(
            src_ref=src, dst_ref=dst, send_sem=send.at[t, kind], recv_sem=recv.at[t, kind],
            device_id={"ep": device}, device_id_type=MESH,
        )

    def to_partner(t):
        return remote(t, 0, dsend.at[t], drecv.at[t], pn)

    def phase_one(t):
        a, b = pl.ds(0, 2), pl.ds(2, 2)
        return (
            remote(t, 1, s1.at[t, a], r1.at[t, a], xn),
            remote(t, 2, s1.at[t, b], r1.at[t, b], yn),
        )

    def phase_two(t):
        return (
            remote(t, 3, s2.at[t, 0], r2.at[t, 0], yn),
            remote(t, 4, s2.at[t, 1], r2.at[t, 1], xn),
        )

    def columns(t):
        return pl.ds(pl.multiple_of(t * width, width), width)

    def w_copy(g):
        slot = lax.rem(g, ring)
        return pltpu.make_async_copy(wd.at[lax.rem(g, own), :, columns(g // own)], wbuf.at[slot], wsem.at[slot])

    def s_copy(t):
        slot = lax.rem(t, 2)
        return pltpu.make_async_copy(sd.at[:, columns(t)], sbuf.at[slot], ssem.at[slot])

    def h_copy(e):
        return pltpu.make_async_copy(h_hbm.at[e], h.at[e], lsem.at[e])

    def y_copy(t):
        slot = lax.rem(t, 2)
        return pltpu.make_async_copy(yst.at[slot], y_hbm.at[:, columns(t)], ysem.at[slot])

    load_ct = pltpu.make_async_copy(ct_hbm, ct, lsem.at[own])
    load_hs = pltpu.make_async_copy(hs_hbm, hs, lsem.at[own + 1])

    for e in range(own):
        h_copy(e).start()
        if e < GROUP:
            w_copy(jnp.int32(e)).start()
    load_ct.start()
    load_hs.start()
    s_copy(jnp.int32(0)).start()
    greet((xn, yn, pn))

    def compute(t):
        @pl.when(t + 1 < tiles)
        def _():
            s_copy(t + 1).start()

        def experts(i, _):
            g = t * own + i * GROUP

            @pl.when(g + GROUP < tiles * own)
            def _():
                for j in range(GROUP):
                    w_copy(g + GROUP + j).start()

            @pl.when(t == 0)
            def _():
                for j in range(GROUP):
                    h_copy(i * GROUP + j).wait()

            for j in range(GROUP):
                w_copy(g + j).wait()
            for j in range(GROUP):
                e = i * GROUP + j
                rows = dot(h[e], wbuf[lax.rem(g + j, ring)]).astype(BF16)
                at = pl.ds(pl.multiple_of(e * PAD, 16), PAD)
                for q in range(8):
                    out[q, at] = rows[q * PAD : (q + 1) * PAD]
            return 0

        lax.fori_loop(0, own // GROUP, experts, 0)

        @pl.when(t == 0)
        def _():
            load_ct.wait()
            load_hs.wait()

        def terms(q):
            return lax.dot_general(ct[q], out[q], (((0,), (0,)), ((), ())), preferred_element_type=F32)

        for q in range(4, 8):
            dsend[t, q - 4] = terms(q).astype(BF16)
        to_partner(t).start()
        s_copy(t).wait()
        keep[t, 0] = terms(0) + dot(hs[...], sbuf[lax.rem(t, 2)])
        for q in range(1, 4):
            keep[t, q] = terms(q)

    def stage_one(t):
        to_partner(t).wait_recv()

        def both(q, rows):
            return keep[t, q, rows] + drecv[t, q, rows].astype(F32)

        s1[t, 0] = both(1, low).astype(BF16)
        s1[t, 1] = both(3, low).astype(BF16)
        s1[t, 2] = both(2, high).astype(BF16)
        s1[t, 3] = both(3, high).astype(BF16)
        for copy in phase_one(t):
            copy.start()
        keep[t, 0] = keep[t, 0] + drecv[t, 0].astype(F32)
        keep[t, 1, high] = both(1, high)
        keep[t, 2, low] = both(2, low)

    def stage_two(t):
        for copy in phase_one(t):
            copy.wait_recv()
        s2[t, 0] = (keep[t, 2, low] + r1[t, 1].astype(F32)).astype(BF16)
        s2[t, 1] = (keep[t, 1, high] + r1[t, 3].astype(F32)).astype(BF16)
        for copy in phase_two(t):
            copy.start()
        keep[t, 0, low] = keep[t, 0, low] + r1[t, 0].astype(F32)
        keep[t, 0, high] = keep[t, 0, high] + r1[t, 2].astype(F32)

    def stage_three(t):
        for copy in phase_two(t):
            copy.wait_recv()

        @pl.when(t >= 2)
        def _():
            y_copy(t - 2).wait()

        slot = lax.rem(t, 2)
        yst[slot, low] = (keep[t, 0, low] + r2[t, 0].astype(F32)).astype(BF16)
        yst[slot, high] = (keep[t, 0, high] + r2[t, 1].astype(F32)).astype(BF16)
        y_copy(t).start()

    def tile(t, _):
        @pl.when(t < tiles)
        def _():
            compute(t)
            stage_one(t)

        @pl.when(jnp.logical_and(t >= 1, t <= tiles))
        def _():
            stage_two(t - 1)

        @pl.when(t >= 2)
        def _():
            stage_three(t - 2)

        return 0

    lax.fori_loop(0, tiles + 2, tile, 0)
    for t in (tiles - 2, tiles - 1):
        y_copy(jnp.int32(t)).wait()

    def drain(t, _):
        for copy in (to_partner(t), *phase_one(t), *phase_two(t)):
            copy.wait_send()
        return 0

    lax.fori_loop(0, tiles, drain, 0)


def solution(mesh):
    members = mesh.shape["ep"]

    def body(x, expert, slot, gate, w_gate, w_up, w_down, s_gate, s_up, s_down):
        tokens, top = expert.shape[2:]
        own, d, ff = w_gate.shape
        slots = 5 * tokens * top // (4 * own * members)
        x, expert, slot, gate = x[0, 0], expert[0, 0], slot[0, 0], gate[0, 0]
        place = jnp.where(slot < slots, expert * PAD + slot, -1).astype(F32)
        fill = ((0, 8 - top), (0, 0))
        meta = jnp.concatenate([jnp.pad(place.T, fill, constant_values=-1.0), jnp.pad(gate.T, fill)])

        hbm = pl.BlockSpec(memory_space=pl.ANY)
        dma = pltpu.SemaphoreType.DMA
        pieces, ring = 8, 2 * GROUP
        width = d // pieces
        rows = own * PAD
        h, hs, ct = pl.pallas_call(
            functools.partial(first_kernel, (pieces, width, tokens, ff, own, ring)),
            out_shape=(
                jax.ShapeDtypeStruct((own, rows, ff), BF16),
                jax.ShapeDtypeStruct((tokens, 2 * ff), BF16),
                jax.ShapeDtypeStruct((8, rows, tokens), BF16),
            ),
            in_specs=[hbm] * 6,
            out_specs=(hbm,) * 3,
            scratch_shapes=[
                pltpu.VMEM((pieces, 8, tokens, width), BF16),
                pltpu.VMEM((8, 16, tokens), F32),
                pltpu.VMEM((own, rows, 2 * ff), F32),
                pltpu.VMEM((ring, width, 2 * ff), BF16),
                pltpu.VMEM((own, rows, width), BF16),
                pltpu.VMEM((8, rows, tokens), BF16),
                pltpu.VMEM((2, rows, ff), BF16),
                pltpu.VMEM((2, rows, tokens), BF16),
                dma((pieces + 1,)),
                dma((ring, 2)),
                dma((2,)),
                dma((2,)),
                dma((pieces + 1, 8)),
                dma((pieces + 1, 8)),
            ],
            compiler_params=pltpu.CompilerParams(
                collective_id=0, has_side_effects=True, vmem_limit_bytes=VMEM_BYTES
            ),
            name="dispatch_up",
        )(x, meta, w_gate, w_up, s_gate, s_up)

        tiles, ring = 8, 2 * GROUP
        width = d // tiles
        y = pl.pallas_call(
            functools.partial(second_kernel, (tiles, width, tokens, own, ring)),
            out_shape=jax.ShapeDtypeStruct((tokens, d), BF16),
            in_specs=[hbm] * 5,
            out_specs=hbm,
            scratch_shapes=[
                pltpu.VMEM((own, rows, ff), BF16),
                pltpu.VMEM((tokens, 2 * ff), BF16),
                pltpu.VMEM((8, rows, tokens), BF16),
                pltpu.VMEM((ring, ff, width), BF16),
                pltpu.VMEM((2, 2 * ff, width), BF16),
                pltpu.VMEM((8, rows, width), BF16),
                pltpu.VMEM((tiles, 4, tokens, width), F32),
                pltpu.VMEM((tiles, 4, tokens, width), BF16),
                pltpu.VMEM((tiles, 4, tokens, width), BF16),
                pltpu.VMEM((tiles, 4, tokens // 2, width), BF16),
                pltpu.VMEM((tiles, 4, tokens // 2, width), BF16),
                pltpu.VMEM((tiles, 2, tokens // 2, width), BF16),
                pltpu.VMEM((tiles, 2, tokens // 2, width), BF16),
                pltpu.VMEM((2, tokens, width), BF16),
                dma((own + 2,)),
                dma((ring,)),
                dma((2,)),
                dma((2,)),
                dma((tiles, 5)),
                dma((tiles, 5)),
            ],
            compiler_params=pltpu.CompilerParams(
                collective_id=1, has_side_effects=True, vmem_limit_bytes=VMEM_BYTES
            ),
            name="down_combine",
        )(h, hs, ct, w_down, s_down)
        return y[None, None]

    tok, exp, rep = P("dp", "ep"), P("ep"), P()
    return jax.shard_map(
        body,
        mesh=mesh,
        in_specs=(tok,) * 4 + (exp,) * 3 + (rep,) * 3,
        out_specs=tok,
        check_vma=False,
    )
```

```python
import functools

import jax
import jax.numpy as jnp
from jax import lax
from jax.experimental import pallas as pl
from jax.experimental.pallas import tpu as pltpu
from jax.sharding import PartitionSpec as P

MESH = pl.DeviceIdType.MESH
F32, BF16 = jnp.float32, jnp.bfloat16
VMEM_BYTES = 67043328
GROUP, BATCH = 4, 4
PAD = 48
OWN, NEAR, FAR, RELAY, LAST, PARTNER = (0, 1, 2), (0, 1), (3, 4), (3, 4, 5, 6), (7,), (2, 5, 6, 7)


def neighbours():
    me = lax.axis_index("ep")
    core, y, x = lax.rem(me, 2), lax.rem(me // 2, 2), me // 4
    return me, me + 4 - 8 * x, me + 2 - 4 * y, me + 1 - 2 * core


def greet(devices):
    barrier = pltpu.get_barrier_semaphore()
    for device in devices:
        pl.semaphore_signal(barrier, inc=1, device_id={"ep": device}, device_id_type=MESH)
    pl.semaphore_wait(barrier, len(devices))


def dot(a, b):
    return jnp.dot(a, b, preferred_element_type=F32)


def spread(width):
    return [(n, min(n + 256, width)) for n in range(0, width, 256)]


def first_kernel(
    dims, x_hbm, meta_hbm, wg, wu, sg, su, h_out, hs_out, ct_out,
    xg, meta, acc, wbuf, z, pm, stage, ctst, xsem, wsem, osem, csem, send, recv,
):
    pieces, width, tokens, ff, own, ring = dims
    me, xn, yn, pn = neighbours()
    half = tokens // 2
    shared_steps = 2 * pieces
    total = shared_steps + pieces * own

    def copies(ref, piece, rows, kinds):
        mid = rows // 2
        low, high = pl.ds(0, mid), pl.ds(mid, mid)
        plan = (
            (ref(0), ref(1), xn), (ref(0), ref(2), yn), (ref(0), ref(4), pn),
            (ref(1).at[low], ref(3).at[low], yn), (ref(2).at[high], ref(3).at[high], xn),
            (ref(1), ref(5), pn), (ref(2), ref(6), pn), (ref(3), ref(7), pn),
        )
        return [
            pltpu.make_async_remote_copy(
                src_ref=src, dst_ref=dst, send_sem=send.at[piece, kind], recv_sem=recv.at[piece, kind],
                device_id={"ep": device}, device_id_type=MESH,
            )
            for kind, (src, dst, device) in enumerate(plan) if kind in kinds
        ]

    def of_x(c, kinds):
        return copies(lambda q: xg.at[c, q], c, tokens, kinds)

    def of_meta(kinds):
        return copies(lambda q: meta.at[q], pieces, 16, kinds)

    def start(group):
        for copy in group:
            copy.start()

    def await_recv(group):
        for copy in group:
            copy.wait_recv()

    def load_x(c):
        return pltpu.make_async_copy(x_hbm.at[:, pl.ds(c * width, width)], xg.at[c, 0], xsem.at[c])

    load_meta = pltpu.make_async_copy(meta_hbm, meta.at[0], xsem.at[pieces])

    def w_copy(src, slot, part):
        return pltpu.make_async_copy(src, wbuf.at[slot, :, pl.ds(part * ff, ff)], wsem.at[slot, part])

    def fetch(g):
        slot = lax.rem(g, ring)

        @pl.when(g < shared_steps)
        def _():
            rows = pl.ds(pl.multiple_of(g // 2 * width, width), width)
            for which, src in enumerate((sg, su)):

                @pl.when(lax.rem(g, 2) == which)
                def _():
                    for part in range(2):
                        w_copy(src.at[rows, pl.ds(part * ff, ff)], slot, part).start()

        @pl.when(jnp.logical_and(g >= shared_steps, g < total))
        def _():
            at = g - shared_steps
            rows = pl.ds(pl.multiple_of(at // own * width, width), width)
            for part, src in enumerate((wg, wu)):
                w_copy(src.at[lax.rem(at, own), rows], slot, part).start()

    def await_w(slot):
        for part in range(2):
            w_copy(wg.at[0, pl.ds(0, width)], slot, part).wait()

    load_meta.start()
    for c in range(pieces):
        load_x(c).start()
    for g in range(ring - GROUP):
        fetch(jnp.int32(g))
    greet((xn, yn, pn))
    load_meta.wait()
    start(of_meta(OWN))
    for c in range(pieces):
        load_x(c).wait()
        if c < 2:
            start(of_x(c, OWN))

    def take(group):
        for i in range(GROUP):
            fetch(group * GROUP + ring - GROUP + i)
        slots = [lax.rem(group * GROUP + i, ring) for i in range(GROUP)]
        for slot in slots:
            await_w(slot)
        return slots

    def shared(p, _, new):
        slots = [slot for i in range(4 // GROUP) for slot in take(p * (4 // GROUP) + i)]
        for which in range(2):
            for n0, n1 in spread(2 * ff):
                terms = sum(dot(xg[2 * p + i, 0], wbuf[slots[2 * i + which], :, n0:n1]) for i in range(2))
                acc[which, :, n0:n1] = terms if new else acc[which, :, n0:n1] + terms
        return 0

    def relay(c):
        await_recv(of_x(c, NEAR))
        start(of_x(c, RELAY))

    shared(0, 0, True)
    await_recv(of_meta(NEAR))
    start(of_meta(RELAY))

    def shared_rest(p, _):
        shared(p, 0, False)

        @pl.when(p == 1)
        def _():
            await_recv(of_meta(FAR))
            start(of_meta(LAST))

        @pl.when(p == 2)
        def _():
            relay(0)
            start(of_x(2, OWN))

        return 0

    lax.fori_loop(1, shared_steps // 4, shared_rest, 0)

    def out_hs(part):
        return pltpu.make_async_copy(stage.at[part], hs_out.at[:, pl.ds(part * ff, ff)], osem.at[part])

    for part in range(2):
        for n0, n1 in spread(ff):
            at = slice(part * ff + n0, part * ff + n1)
            stage[part, :, n0:n1] = (jax.nn.silu(acc[0, :, at]) * acc[1, :, at]).astype(BF16)
        out_hs(part).start()

    await_recv(of_meta(PARTNER))
    base = (me * (own * PAD)).astype(F32)
    row = lax.broadcasted_iota(jnp.int32, (PAD, tokens), 0).astype(F32)

    def out_ct(q):
        return pltpu.make_async_copy(ctst.at[lax.rem(q, 2)], ct_out.at[q], csem.at[lax.rem(q, 2)])

    def one_hot(q, _):
        @pl.when(q >= 2)
        def _():
            out_ct(q - 2).wait()

        place, gate = meta[q, 0:8] - base, meta[q, 8:16]
        for e in range(own):
            p = jnp.zeros((PAD, tokens), F32)
            c = jnp.zeros((PAD, tokens), F32)
            for j in range(6):
                hit = (place[j : j + 1] - float(e * PAD)) == row
                p = jnp.where(hit, 1.0, p)
                c = jnp.where(hit, gate[j : j + 1], c)
            pm[q, e * PAD : (e + 1) * PAD] = p.astype(BF16)
            ctst[lax.rem(q, 2), e * PAD : (e + 1) * PAD] = c.astype(BF16)
        out_ct(q).start()
        return 0

    lax.fori_loop(0, 8, one_hot, 0)
    for q in (6, 7):
        out_ct(jnp.int32(q)).wait()
    for part in range(2):
        out_hs(part).wait()

    def gather(c):
        def place_rows(q):
            rows = dot(pm[q], xg[c, q]).astype(BF16)
            for e in range(own):
                z[e, q * PAD : (q + 1) * PAD] = rows[e * PAD : (e + 1) * PAD]

        await_recv(of_x(c, PARTNER))
        for q in range(8):
            place_rows(q)

    def pass_on(c):
        @pl.when(c + 1 < pieces)
        def _():
            relay(c + 1)

        @pl.when(c + 3 < pieces)
        def _():
            start(of_x(c + 3, OWN))

        await_recv(of_x(c, FAR))
        start(of_x(c, LAST))

    def piece(c, _, new):
        def experts(i, _):
            @pl.when(i == 1)
            def _():
                pass_on(c + 1)

            slots = take((shared_steps + c * own) // GROUP + i)
            for j, slot in enumerate(slots):
                e = i * GROUP + j
                lhs = z[e]
                for n0, n1 in spread(2 * ff):
                    term = dot(lhs, wbuf[slot, :, n0:n1])
                    acc[e, :, n0:n1] = term if new else acc[e, :, n0:n1] + term
            return 0

        lax.fori_loop(0, own // GROUP, experts, 0)
        gather(c + 1)
        return 0

    pass_on(jnp.int32(0))
    gather(0)
    piece(jnp.int32(0), 0, True)
    lax.fori_loop(1, pieces - 1, functools.partial(piece, new=False), 0)

    last = pieces - 1

    def out_h(e):
        return pltpu.make_async_copy(stage.at[lax.rem(e, 2)], h_out.at[e], osem.at[lax.rem(e, 2)])

    def finish(i, _):
        slots = take((shared_steps + last * own) // GROUP + i)
        for j, slot in enumerate(slots):
            e = i * GROUP + j
            if j >= 2:
                out_h(e - 2).wait()
            else:

                @pl.when(i > 0)
                def _():
                    out_h(e - 2).wait()

            lhs = z[e]
            for n0, n1 in spread(ff):
                a = acc[e, :, n0:n1] + dot(lhs, wbuf[slot, :, n0:n1])
                b = acc[e, :, ff + n0 : ff + n1] + dot(lhs, wbuf[slot, :, ff + n0 : ff + n1])
                stage[j % 2, :, n0:n1] = (jax.nn.silu(a) * b).astype(BF16)
            out_h(e).start()
        return 0

    lax.fori_loop(0, own // GROUP, finish, 0)
    for e in (own - 2, own - 1):
        out_h(jnp.int32(e)).wait()

    def drain(c, _):
        for copy in of_x(c, range(8)):
            copy.wait_send()
        return 0

    lax.fori_loop(0, pieces, drain, 0)
    for copy in of_meta(range(8)):
        copy.wait_send()


def second_kernel(
    dims, h_hbm, hs_hbm, ct_hbm, wd, sd, y_hbm,
    h, hs, ct, wbuf, sbuf, out, keep, dsend, drecv, s1, r1, s2, r2, yst,
    lsem, wsem, ssem, ysem, send, recv,
):
    tiles, width, tokens, own, ring = dims
    me, xn, yn, pn = neighbours()
    half = tokens // 2
    low, high = pl.ds(0, half), pl.ds(half, half)

    def remote(t, kind, src, dst, device):
        return pltpu.make_async_remote_copy(
            src_ref=src, dst_ref=dst, send_sem=send.at[t, kind], recv_sem=recv.at[t, kind],
            device_id={"ep": device}, device_id_type=MESH,
        )

    def to_partner(t):
        return remote(t, 0, dsend.at[t], drecv.at[t], pn)

    def phase_one(t):
        a, b = pl.ds(0, 2), pl.ds(2, 2)
        return (
            remote(t, 1, s1.at[t, a], r1.at[t, a], xn),
            remote(t, 2, s1.at[t, b], r1.at[t, b], yn),
        )

    def phase_two(t):
        return (
            remote(t, 3, s2.at[t, 0], r2.at[t, 0], yn),
            remote(t, 4, s2.at[t, 1], r2.at[t, 1], xn),
        )

    def columns(t):
        return pl.ds(pl.multiple_of(t * width, width), width)

    def w_copy(g):
        slot = lax.rem(g, ring)
        return pltpu.make_async_copy(wd.at[lax.rem(g, own), :, columns(g // own)], wbuf.at[slot], wsem.at[slot])

    def s_copy(t):
        slot = lax.rem(t, 2)
        return pltpu.make_async_copy(sd.at[:, columns(t)], sbuf.at[slot], ssem.at[slot])

    def h_copy(e):
        return pltpu.make_async_copy(h_hbm.at[e], h.at[e], lsem.at[e])

    def y_copy(t):
        slot = lax.rem(t, 2)
        return pltpu.make_async_copy(yst.at[slot], y_hbm.at[:, columns(t)], ysem.at[slot])

    load_ct = pltpu.make_async_copy(ct_hbm, ct, lsem.at[own])
    load_hs = pltpu.make_async_copy(hs_hbm, hs, lsem.at[own + 1])

    for e in range(own):
        h_copy(e).start()
        if e < ring - BATCH:
            w_copy(jnp.int32(e)).start()
    load_ct.start()
    load_hs.start()
    s_copy(jnp.int32(0)).start()
    greet((xn, yn, pn))

    def compute(t):
        @pl.when(t + 1 < tiles)
        def _():
            s_copy(t + 1).start()

        def experts(i, _):
            @pl.when(jnp.logical_and(i == 1, t >= 1))
            def _():
                stage_one(t - 1)

            g = t * own + i * BATCH

            @pl.when(g + ring - BATCH < tiles * own)
            def _():
                for j in range(BATCH):
                    w_copy(g + ring - BATCH + j).start()

            @pl.when(t == 0)
            def _():
                for j in range(BATCH):
                    h_copy(i * BATCH + j).wait()

            for j in range(BATCH):
                w_copy(g + j).wait()
            for j in range(BATCH):
                e = i * BATCH + j
                rows = dot(h[e], wbuf[lax.rem(g + j, ring)]).astype(BF16)
                at = pl.ds(pl.multiple_of(e * PAD, 16), PAD)
                for q in range(8):
                    out[q, at] = rows[q * PAD : (q + 1) * PAD]
            return 0

        lax.fori_loop(0, own // BATCH, experts, 0)

        @pl.when(t >= 2)
        def _():
            stage_two(t - 2)

        @pl.when(t == 0)
        def _():
            load_ct.wait()
            load_hs.wait()

        def terms(q):
            return lax.dot_general(ct[q], out[q], (((0,), (0,)), ((), ())), preferred_element_type=F32)

        for q in range(4, 8):
            dsend[t, q - 4] = terms(q).astype(BF16)
        to_partner(t).start()
        s_copy(t).wait()
        keep[t, 0] = terms(0) + dot(hs[...], sbuf[lax.rem(t, 2)])
        for q in range(1, 4):
            keep[t, q] = terms(q)

    def stage_one(t):
        to_partner(t).wait_recv()

        def both(q, rows):
            return keep[t, q, rows] + drecv[t, q, rows].astype(F32)

        s1[t, 0] = both(1, low).astype(BF16)
        s1[t, 1] = both(3, low).astype(BF16)
        s1[t, 2] = both(2, high).astype(BF16)
        s1[t, 3] = both(3, high).astype(BF16)
        for copy in phase_one(t):
            copy.start()
        keep[t, 0] = keep[t, 0] + drecv[t, 0].astype(F32)
        keep[t, 1, high] = both(1, high)
        keep[t, 2, low] = both(2, low)

    def stage_two(t):
        for copy in phase_one(t):
            copy.wait_recv()
        s2[t, 0] = (keep[t, 2, low] + r1[t, 1].astype(F32)).astype(BF16)
        s2[t, 1] = (keep[t, 1, high] + r1[t, 3].astype(F32)).astype(BF16)
        for copy in phase_two(t):
            copy.start()
        keep[t, 0, low] = keep[t, 0, low] + r1[t, 0].astype(F32)
        keep[t, 0, high] = keep[t, 0, high] + r1[t, 2].astype(F32)

    def stage_three(t):
        for copy in phase_two(t):
            copy.wait_recv()

        @pl.when(t >= 2)
        def _():
            y_copy(t - 2).wait()

        slot = lax.rem(t, 2)
        yst[slot, low] = (keep[t, 0, low] + r2[t, 0].astype(F32)).astype(BF16)
        yst[slot, high] = (keep[t, 0, high] + r2[t, 1].astype(F32)).astype(BF16)
        y_copy(t).start()

    def tile(t, _):
        @pl.when(t < tiles)
        def _():
            compute(t)

        @pl.when(t == tiles)
        def _():
            stage_one(t - 1)

        @pl.when(jnp.logical_and(t >= tiles, t <= tiles + 1))
        def _():
            stage_two(t - 2)

        @pl.when(t >= 3)
        def _():
            stage_three(t - 3)

        return 0

    lax.fori_loop(0, tiles + 3, tile, 0)
    for t in (tiles - 2, tiles - 1):
        y_copy(jnp.int32(t)).wait()

    def drain(t, _):
        for copy in (to_partner(t), *phase_one(t), *phase_two(t)):
            copy.wait_send()
        return 0

    lax.fori_loop(0, tiles, drain, 0)


def solution(mesh):
    members = mesh.shape["ep"]

    def body(x, expert, slot, gate, w_gate, w_up, w_down, s_gate, s_up, s_down):
        tokens, top = expert.shape[2:]
        own, d, ff = w_gate.shape
        slots = 5 * tokens * top // (4 * own * members)
        x, expert, slot, gate = x[0, 0], expert[0, 0], slot[0, 0], gate[0, 0]
        place = jnp.where(slot < slots, expert * PAD + slot, -1).astype(F32)
        fill = ((0, 8 - top), (0, 0))
        meta = jnp.concatenate([jnp.pad(place.T, fill, constant_values=-1.0), jnp.pad(gate.T, fill)])

        hbm = pl.BlockSpec(memory_space=pl.ANY)
        dma = pltpu.SemaphoreType.DMA
        pieces, ring = 8, 8
        width = d // pieces
        rows = own * PAD
        h, hs, ct = pl.pallas_call(
            functools.partial(first_kernel, (pieces, width, tokens, ff, own, ring)),
            out_shape=(
                jax.ShapeDtypeStruct((own, rows, ff), BF16),
                jax.ShapeDtypeStruct((tokens, 2 * ff), BF16),
                jax.ShapeDtypeStruct((8, rows, tokens), BF16),
            ),
            in_specs=[hbm] * 6,
            out_specs=(hbm,) * 3,
            scratch_shapes=[
                pltpu.VMEM((pieces, 8, tokens, width), BF16),
                pltpu.VMEM((8, 16, tokens), F32),
                pltpu.VMEM((own, rows, 2 * ff), F32),
                pltpu.VMEM((ring, width, 2 * ff), BF16),
                pltpu.VMEM((own, rows, width), BF16),
                pltpu.VMEM((8, rows, tokens), BF16),
                pltpu.VMEM((2, rows, ff), BF16),
                pltpu.VMEM((2, rows, tokens), BF16),
                dma((pieces + 1,)),
                dma((ring, 2)),
                dma((2,)),
                dma((2,)),
                dma((pieces + 1, 8)),
                dma((pieces + 1, 8)),
            ],
            compiler_params=pltpu.CompilerParams(
                collective_id=0, has_side_effects=True, vmem_limit_bytes=VMEM_BYTES
            ),
            name="dispatch_up",
        )(x, meta, w_gate, w_up, s_gate, s_up)

        tiles, ring = 8, 12
        width = d // tiles
        y = pl.pallas_call(
            functools.partial(second_kernel, (tiles, width, tokens, own, ring)),
            out_shape=jax.ShapeDtypeStruct((tokens, d), BF16),
            in_specs=[hbm] * 5,
            out_specs=hbm,
            scratch_shapes=[
                pltpu.VMEM((own, rows, ff), BF16),
                pltpu.VMEM((tokens, 2 * ff), BF16),
                pltpu.VMEM((8, rows, tokens), BF16),
                pltpu.VMEM((ring, ff, width), BF16),
                pltpu.VMEM((2, 2 * ff, width), BF16),
                pltpu.VMEM((8, rows, width), BF16),
                pltpu.VMEM((tiles, 4, tokens, width), F32),
                pltpu.VMEM((tiles, 4, tokens, width), BF16),
                pltpu.VMEM((tiles, 4, tokens, width), BF16),
                pltpu.VMEM((tiles, 4, tokens // 2, width), BF16),
                pltpu.VMEM((tiles, 4, tokens // 2, width), BF16),
                pltpu.VMEM((tiles, 2, tokens // 2, width), BF16),
                pltpu.VMEM((tiles, 2, tokens // 2, width), BF16),
                pltpu.VMEM((2, tokens, width), BF16),
                dma((own + 2,)),
                dma((ring,)),
                dma((2,)),
                dma((2,)),
                dma((tiles, 5)),
                dma((tiles, 5)),
            ],
            compiler_params=pltpu.CompilerParams(
                collective_id=1, has_side_effects=True, vmem_limit_bytes=VMEM_BYTES
            ),
            name="down_combine",
        )(h, hs, ct, w_down, s_down)
        return y[None, None]

    tok, exp, rep = P("dp", "ep"), P("ep"), P()
    return jax.shard_map(
        body,
        mesh=mesh,
        in_specs=(tok,) * 4 + (exp,) * 3 + (rep,) * 3,
        out_specs=tok,
        check_vma=False,
    )
```

```python
import functools

import jax
import jax.numpy as jnp
from jax import lax
from jax.experimental import pallas as pl
from jax.experimental.pallas import tpu as pltpu
from jax.sharding import PartitionSpec as P

MESH = pl.DeviceIdType.MESH
F32, BF16 = jnp.float32, jnp.bfloat16
VMEM_BYTES = 67043328
GROUP, BATCH = 4, 4
PAD = 48
OWN, NEAR, FAR, RELAY, LAST, PARTNER = (0, 1, 2), (0, 1), (3, 4), (3, 4, 5, 6), (7,), (2, 5, 6, 7)


def neighbours():
    me = lax.axis_index("ep")
    core, y, x = lax.rem(me, 2), lax.rem(me // 2, 2), me // 4
    return me, me + 4 - 8 * x, me + 2 - 4 * y, me + 1 - 2 * core


def greet(devices):
    barrier = pltpu.get_barrier_semaphore()
    for device in devices:
        pl.semaphore_signal(barrier, inc=1, device_id={"ep": device}, device_id_type=MESH)
    pl.semaphore_wait(barrier, len(devices))


def dot(a, b):
    return jnp.dot(a, b, preferred_element_type=F32)


def spread(width):
    return [(n, min(n + 256, width)) for n in range(0, width, 256)]


def first_kernel(
    dims, x_hbm, meta_hbm, wg, wu, h_out, ct_out,
    xg, meta, acc, wbuf, z, pm, stage, ctst, xsem, wsem, osem, csem, send, recv,
):
    pieces, width, tokens, ff, own, ring = dims
    me, xn, yn, pn = neighbours()
    dn = xn + yn - me
    others = [xn, yn, dn] + [device + pn - me for device in (me, xn, yn, dn)]
    total = pieces * own

    def copies(ref, piece, rows, kinds):
        mid = rows // 2
        low, high = pl.ds(0, mid), pl.ds(mid, mid)
        plan = (
            (ref(0), ref(1), xn), (ref(0), ref(2), yn), (ref(0), ref(4), pn),
            (ref(1).at[low], ref(3).at[low], yn), (ref(2).at[high], ref(3).at[high], xn),
            (ref(1), ref(5), pn), (ref(2), ref(6), pn), (ref(3), ref(7), pn),
        )
        return [
            pltpu.make_async_remote_copy(
                src_ref=src, dst_ref=dst, send_sem=send.at[piece, kind], recv_sem=recv.at[piece, kind],
                device_id={"ep": device}, device_id_type=MESH,
            )
            for kind, (src, dst, device) in enumerate(plan) if kind in kinds
        ]

    def of_x(c, kinds):
        return copies(lambda q: xg.at[c, q], c, tokens, kinds)

    def of_meta():
        return [
            pltpu.make_async_remote_copy(
                src_ref=meta.at[0], dst_ref=meta.at[q + 1], send_sem=send.at[pieces, q], recv_sem=recv.at[pieces, q],
                device_id={"ep": device}, device_id_type=MESH,
            )
            for q, device in enumerate(others)
        ]

    def start(group):
        for copy in group:
            copy.start()

    def await_recv(group):
        for copy in group:
            copy.wait_recv()

    def load_x(c):
        return pltpu.make_async_copy(x_hbm.at[:, pl.ds(c * width, width)], xg.at[c, 0], xsem.at[c])

    load_meta = pltpu.make_async_copy(meta_hbm, meta.at[0], xsem.at[pieces])

    def w_copy(src, slot, part):
        return pltpu.make_async_copy(src, wbuf.at[slot, :, pl.ds(part * ff, ff)], wsem.at[slot, part])

    def fetch(g):
        slot = lax.rem(g, ring)

        @pl.when(g < total)
        def _():
            rows = pl.ds(pl.multiple_of(g // own * width, width), width)
            for part, src in enumerate((wg, wu)):
                w_copy(src.at[lax.rem(g, own), rows], slot, part).start()

    def await_w(slot):
        for part in range(2):
            w_copy(wg.at[0, pl.ds(0, width)], slot, part).wait()

    load_meta.start()
    for c in range(pieces):
        load_x(c).start()
    greet(others)
    load_meta.wait()
    start(of_meta())
    load_x(0).wait()
    start(of_x(0, OWN))
    for g in range(ring - GROUP):
        fetch(jnp.int32(g))
    for c in range(1, pieces):
        load_x(c).wait()

    def take(group):
        for i in range(GROUP):
            fetch(group * GROUP + ring - GROUP + i)
        slots = [lax.rem(group * GROUP + i, ring) for i in range(GROUP)]
        for slot in slots:
            await_w(slot)
        return slots

    def relay(c):
        await_recv(of_x(c, NEAR))
        start(of_x(c, RELAY))

    await_recv(of_meta())
    base = (me * (own * PAD)).astype(F32)
    row = lax.broadcasted_iota(jnp.int32, (PAD, tokens), 0).astype(F32)

    def out_ct(q):
        return pltpu.make_async_copy(ctst.at[lax.rem(q, 2)], ct_out.at[q], csem.at[lax.rem(q, 2)])

    def one_hot(q, _):
        @pl.when(q >= 2)
        def _():
            out_ct(q - 2).wait()

        place, gate = meta[q, 0:8] - base, meta[q, 8:16]
        for e in range(own):
            p = jnp.zeros((PAD, tokens), F32)
            c = jnp.zeros((PAD, tokens), F32)
            for j in range(6):
                hit = (place[j : j + 1] - float(e * PAD)) == row
                p = jnp.where(hit, 1.0, p)
                c = jnp.where(hit, gate[j : j + 1], c)
            pm[q, e * PAD : (e + 1) * PAD] = p.astype(BF16)
            ctst[lax.rem(q, 2), e * PAD : (e + 1) * PAD] = c.astype(BF16)
        out_ct(q).start()
        return 0

    lax.fori_loop(0, 8, one_hot, 0)
    for q in (6, 7):
        out_ct(jnp.int32(q)).wait()

    def gather(c):
        def place_rows(q):
            rows = dot(pm[q], xg[c, q]).astype(BF16)
            for e in range(own):
                z[e, q * PAD : (q + 1) * PAD] = rows[e * PAD : (e + 1) * PAD]

        await_recv(of_x(c, PARTNER))
        for q in range(8):
            place_rows(q)

    def pass_on(c):
        @pl.when(c + 1 < pieces)
        def _():
            relay(c + 1)

        @pl.when(c + 3 < pieces)
        def _():
            start(of_x(c + 3, OWN))

        await_recv(of_x(c, FAR))
        start(of_x(c, LAST))

    def piece(c, _, new):
        def experts(i, _):
            @pl.when(i == 1)
            def _():
                if new:
                    relay(1)
                    start(of_x(3, OWN))
                else:
                    pass_on(c + 1)

            slots = take(c * own // GROUP + i)
            for j, slot in enumerate(slots):
                e = i * GROUP + j
                lhs = z[e]
                for n0, n1 in spread(2 * ff):
                    term = dot(lhs, wbuf[slot, :, n0:n1])
                    acc[e, :, n0:n1] = term if new else acc[e, :, n0:n1] + term
            return 0

        lax.fori_loop(0, own // GROUP, experts, 0)
        if new:
            pass_on(c + 1)
        gather(c + 1)
        return 0

    relay(0)
    for c in (1, 2):
        start(of_x(c, OWN))
    await_recv(of_x(0, FAR))
    start(of_x(0, LAST))
    gather(0)
    piece(jnp.int32(0), 0, True)
    lax.fori_loop(1, pieces - 1, functools.partial(piece, new=False), 0)

    last = pieces - 1

    def out_h(e):
        return pltpu.make_async_copy(stage.at[lax.rem(e, 2)], h_out.at[e], osem.at[lax.rem(e, 2)])

    def finish(i, _):
        slots = take(last * own // GROUP + i)
        for j, slot in enumerate(slots):
            e = i * GROUP + j
            if j >= 2:
                out_h(e - 2).wait()
            else:

                @pl.when(i > 0)
                def _():
                    out_h(e - 2).wait()

            lhs = z[e]
            for n0, n1 in spread(ff):
                a = acc[e, :, n0:n1] + dot(lhs, wbuf[slot, :, n0:n1])
                b = acc[e, :, ff + n0 : ff + n1] + dot(lhs, wbuf[slot, :, ff + n0 : ff + n1])
                stage[j % 2, :, n0:n1] = (jax.nn.silu(a) * b).astype(BF16)
            out_h(e).start()
        return 0

    lax.fori_loop(0, own // GROUP, finish, 0)
    for e in (own - 2, own - 1):
        out_h(jnp.int32(e)).wait()

    def drain(c, _):
        for copy in of_x(c, range(8)):
            copy.wait_send()
        return 0

    lax.fori_loop(0, pieces, drain, 0)
    for copy in of_meta():
        copy.wait_send()


def second_kernel(
    dims, h_hbm, ct_hbm, x_hbm, wd, sg, su, sd, y_hbm,
    h, ct, x, hs, wbuf, ubuf, sbuf, out, keep, dsend, drecv, s1, r1, s2, r2, yst,
    lsem, wsem, usem, ssem, ysem, send, recv,
):
    tiles, width, tokens, own, ring = dims
    me, xn, yn, pn = neighbours()
    half = tokens // 2
    low, high = pl.ds(0, half), pl.ds(half, half)
    slices = hs.shape[1] // width

    def remote(t, kind, src, dst, device):
        return pltpu.make_async_remote_copy(
            src_ref=src, dst_ref=dst, send_sem=send.at[t, kind], recv_sem=recv.at[t, kind],
            device_id={"ep": device}, device_id_type=MESH,
        )

    def to_partner(t):
        return remote(t, 0, dsend.at[lax.rem(t, 3)], drecv.at[t], pn)

    def phase_one(t):
        a, b = pl.ds(0, 2), pl.ds(2, 2)
        return (
            remote(t, 1, s1.at[t, a], r1.at[t, a], xn),
            remote(t, 2, s1.at[t, b], r1.at[t, b], yn),
        )

    def phase_two(t):
        return (
            remote(t, 3, s2.at[t, 0], r2.at[t, 0], yn),
            remote(t, 4, s2.at[t, 1], r2.at[t, 1], xn),
        )

    def columns(t):
        return pl.ds(pl.multiple_of(t * width, width), width)

    def w_copy(g):
        slot = lax.rem(g, ring)
        return pltpu.make_async_copy(wd.at[lax.rem(g, own), :, columns(g // own)], wbuf.at[slot], wsem.at[slot])

    def s_copy(t):
        slot = lax.rem(t, 2)
        return pltpu.make_async_copy(sd.at[:, columns(t)], sbuf.at[slot], ssem.at[slot])

    def u_copies(j):
        slot = lax.rem(j, 2)
        return [
            pltpu.make_async_copy(src.at[:, columns(j)], ubuf.at[slot, part], usem.at[slot, part])
            for part, src in enumerate((sg, su))
        ]

    def h_copy(e):
        return pltpu.make_async_copy(h_hbm.at[e], h.at[e], lsem.at[e])

    def y_copy(t):
        slot = lax.rem(t, 2)
        return pltpu.make_async_copy(yst.at[slot], y_hbm.at[:, columns(t)], ysem.at[slot])

    load_ct = pltpu.make_async_copy(ct_hbm, ct, lsem.at[own])
    load_x = pltpu.make_async_copy(x_hbm, x, lsem.at[own + 1])

    for e in range(own):
        h_copy(e).start()
        if e < ring - BATCH:
            w_copy(jnp.int32(e)).start()
    load_ct.start()
    greet((xn, yn, pn))

    def compute(t):
        def experts(i, _):
            @pl.when(jnp.logical_and(i == 1, t >= 1))
            def _():
                stage_one(t - 1)

            g = t * own + i * BATCH

            @pl.when(g + ring - BATCH < tiles * own)
            def _():
                for j in range(BATCH):
                    w_copy(g + ring - BATCH + j).start()

            @pl.when(t == 0)
            def _():
                for j in range(BATCH):
                    h_copy(i * BATCH + j).wait()

            for j in range(BATCH):
                w_copy(g + j).wait()
            for j in range(BATCH):
                e = i * BATCH + j
                rows = dot(h[e], wbuf[lax.rem(g + j, ring)]).astype(BF16)
                at = pl.ds(pl.multiple_of(e * PAD, 16), PAD)
                for q in range(8):
                    out[q, at] = rows[q * PAD : (q + 1) * PAD]
            return 0

        lax.fori_loop(0, own // BATCH, experts, 0)

        @pl.when(t >= 2)
        def _():
            stage_two(t - 2)

        @pl.when(t == 0)
        def _():
            load_x.start()
            for j in range(2):
                for copy in u_copies(jnp.int32(j)):
                    copy.start()
                s_copy(jnp.int32(j)).start()
            load_ct.wait()

        def terms(q):
            return lax.dot_general(ct[q], out[q], (((0,), (0,)), ((), ())), preferred_element_type=F32)

        @pl.when(t >= 3)
        def _():
            to_partner(t - 3).wait_send()

        for q in range(4, 8):
            dsend[lax.rem(t, 3), q - 4] = terms(q).astype(BF16)
        to_partner(t).start()
        for q in range(4):
            keep[t, q] = terms(q)

    def shared_up(j):
        for copy in u_copies(j):
            copy.wait()
        slot = lax.rem(j, 2)
        a, b = (dot(x[...], ubuf[slot, part]) for part in range(2))
        hs[:, columns(j)] = (jax.nn.silu(a) * b).astype(BF16)

        @pl.when(j + 2 < slices)
        def _():
            for copy in u_copies(j + 2):
                copy.start()

    def shared_down(t):
        s_copy(t).wait()
        keep[t, 0] = keep[t, 0] + dot(hs[...], sbuf[lax.rem(t, 2)])

        @pl.when(t + 2 < tiles)
        def _():
            s_copy(t + 2).start()

    def stage_one(t):
        to_partner(t).wait_recv()

        def both(q, rows):
            return keep[t, q, rows] + drecv[t, q, rows].astype(F32)

        s1[t, 0] = both(1, low).astype(BF16)
        s1[t, 1] = both(3, low).astype(BF16)
        s1[t, 2] = both(2, high).astype(BF16)
        s1[t, 3] = both(3, high).astype(BF16)
        for copy in phase_one(t):
            copy.start()
        keep[t, 0] = keep[t, 0] + drecv[t, 0].astype(F32)
        keep[t, 1, high] = both(1, high)
        keep[t, 2, low] = both(2, low)

    def stage_two(t):
        for copy in phase_one(t):
            copy.wait_recv()
        s2[t, 0] = (keep[t, 2, low] + r1[t, 1].astype(F32)).astype(BF16)
        s2[t, 1] = (keep[t, 1, high] + r1[t, 3].astype(F32)).astype(BF16)
        for copy in phase_two(t):
            copy.start()
        keep[t, 0, low] = keep[t, 0, low] + r1[t, 0].astype(F32)
        keep[t, 0, high] = keep[t, 0, high] + r1[t, 2].astype(F32)

    def stage_three(t):
        for copy in phase_two(t):
            copy.wait_recv()

        @pl.when(t >= 2)
        def _():
            y_copy(t - 2).wait()

        slot = lax.rem(t, 2)
        yst[slot, low] = (keep[t, 0, low] + r2[t, 0].astype(F32)).astype(BF16)
        yst[slot, high] = (keep[t, 0, high] + r2[t, 1].astype(F32)).astype(BF16)
        y_copy(t).start()

    def tile(t, _):
        @pl.when(t < tiles)
        def _():
            compute(t)

        @pl.when(t == 1)
        def _():
            load_x.wait()

        @pl.when(jnp.logical_and(t >= 1, t < tiles - 1))
        def _():
            for i in range(2):

                @pl.when(2 * t - 2 + i < slices)
                def _():
                    shared_up(2 * t - 2 + i)

        @pl.when(t == tiles)
        def _():
            stage_one(t - 1)

        late = 2 * (t - (tiles - 1))

        @pl.when(late >= 0)
        def _():
            shared_down(late)
            shared_down(late + 1)

        @pl.when(jnp.logical_and(t >= tiles, t <= tiles + 1))
        def _():
            stage_two(t - 2)

        @pl.when(late >= 0)
        def _():
            stage_three(late)
            stage_three(late + 1)

        return 0

    lax.fori_loop(0, tiles + 3, tile, 0)
    for t in (tiles - 2, tiles - 1):
        y_copy(jnp.int32(t)).wait()

    def drain(t, _):
        for copy in (*phase_one(t), *phase_two(t)):
            copy.wait_send()
        return 0

    for t in range(tiles - 3, tiles):
        to_partner(jnp.int32(t)).wait_send()

    lax.fori_loop(0, tiles, drain, 0)


def solution(mesh):
    members = mesh.shape["ep"]

    def body(x, expert, slot, gate, w_gate, w_up, w_down, s_gate, s_up, s_down):
        tokens, top = expert.shape[2:]
        own, d, ff = w_gate.shape
        slots = 5 * tokens * top // (4 * own * members)
        x, expert, slot, gate = x[0, 0], expert[0, 0], slot[0, 0], gate[0, 0]
        place = jnp.where(slot < slots, expert * PAD + slot, -1).astype(F32)
        fill = ((0, 8 - top), (0, 0))
        meta = jnp.concatenate([jnp.pad(place.T, fill, constant_values=-1.0), jnp.pad(gate.T, fill)])

        hbm = pl.BlockSpec(memory_space=pl.ANY)
        dma = pltpu.SemaphoreType.DMA
        pieces, ring = 8, 8
        width = d // pieces
        rows = own * PAD
        h, ct = pl.pallas_call(
            functools.partial(first_kernel, (pieces, width, tokens, ff, own, ring)),
            out_shape=(
                jax.ShapeDtypeStruct((own, rows, ff), BF16),
                jax.ShapeDtypeStruct((8, rows, tokens), BF16),
            ),
            in_specs=[hbm] * 4,
            out_specs=(hbm,) * 2,
            scratch_shapes=[
                pltpu.VMEM((pieces, 8, tokens, width), BF16),
                pltpu.VMEM((8, 16, tokens), F32),
                pltpu.VMEM((own, rows, 2 * ff), F32),
                pltpu.VMEM((ring, width, 2 * ff), BF16),
                pltpu.VMEM((own, rows, width), BF16),
                pltpu.VMEM((8, rows, tokens), BF16),
                pltpu.VMEM((2, rows, ff), BF16),
                pltpu.VMEM((2, rows, tokens), BF16),
                dma((pieces + 1,)),
                dma((ring, 2)),
                dma((2,)),
                dma((2,)),
                dma((pieces + 1, 8)),
                dma((pieces + 1, 8)),
            ],
            compiler_params=pltpu.CompilerParams(
                collective_id=0, has_side_effects=True, vmem_limit_bytes=VMEM_BYTES
            ),
            name="dispatch_up",
        )(x, meta, w_gate, w_up)

        tiles, ring = 8, 12
        width = d // tiles
        y = pl.pallas_call(
            functools.partial(second_kernel, (tiles, width, tokens, own, ring)),
            out_shape=jax.ShapeDtypeStruct((tokens, d), BF16),
            in_specs=[hbm] * 7,
            out_specs=hbm,
            scratch_shapes=[
                pltpu.VMEM((own, rows, ff), BF16),
                pltpu.VMEM((8, rows, tokens), BF16),
                pltpu.VMEM((tokens, d), BF16),
                pltpu.VMEM((tokens, 2 * ff), BF16),
                pltpu.VMEM((ring, ff, width), BF16),
                pltpu.VMEM((2, 2, d, width), BF16),
                pltpu.VMEM((2, 2 * ff, width), BF16),
                pltpu.VMEM((8, rows, width), BF16),
                pltpu.VMEM((tiles, 4, tokens, width), F32),
                pltpu.VMEM((3, 4, tokens, width), BF16),
                pltpu.VMEM((tiles, 4, tokens, width), BF16),
                pltpu.VMEM((tiles, 4, tokens // 2, width), BF16),
                pltpu.VMEM((tiles, 4, tokens // 2, width), BF16),
                pltpu.VMEM((tiles, 2, tokens // 2, width), BF16),
                pltpu.VMEM((tiles, 2, tokens // 2, width), BF16),
                pltpu.VMEM((2, tokens, width), BF16),
                dma((own + 2,)),
                dma((ring,)),
                dma((2, 2)),
                dma((2,)),
                dma((2,)),
                dma((tiles, 5)),
                dma((tiles, 5)),
            ],
            compiler_params=pltpu.CompilerParams(
                collective_id=1, has_side_effects=True, vmem_limit_bytes=VMEM_BYTES
            ),
            name="down_combine",
        )(h, ct, x, w_down, s_gate, s_up, s_down)
        return y[None, None]

    tok, exp, rep = P("dp", "ep"), P("ep"), P()
    return jax.shard_map(
        body,
        mesh=mesh,
        in_specs=(tok,) * 4 + (exp,) * 3 + (rep,) * 3,
        out_specs=tok,
        check_vma=False,
    )
```

```python
import functools

import jax
import jax.numpy as jnp
from jax import lax
from jax.experimental import pallas as pl
from jax.experimental.pallas import tpu as pltpu
from jax.sharding import PartitionSpec as P

MESH = pl.DeviceIdType.MESH
F32, BF16 = jnp.float32, jnp.bfloat16
VMEM_BYTES = 67043328
GROUP, BATCH = 4, 4
PAD = 48
OWN_A, OWN_B, RELAY, FORWARD, LAST, PARTNER = (0, 2, 4), (1, 3), (5, 6), (7, 8), (9,), (4, 7, 8, 9)
NEAR_A, NEAR_B, FAR = (0, 2), (1, 3), (5, 6)


def neighbours():
    me = lax.axis_index("ep")
    core, y, x = lax.rem(me, 2), lax.rem(me // 2, 2), me // 4
    return me, me + 4 - 8 * x, me + 2 - 4 * y, me + 1 - 2 * core


def greet(devices):
    barrier = pltpu.get_barrier_semaphore()
    for device in devices:
        pl.semaphore_signal(barrier, inc=1, device_id={"ep": device}, device_id_type=MESH)
    pl.semaphore_wait(barrier, len(devices))


def dot(a, b):
    return jnp.dot(a, b, preferred_element_type=F32)


def spread(width):
    return [(n, min(n + 256, width)) for n in range(0, width, 256)]


def first_kernel(
    dims, x_hbm, meta_hbm, wg, wu, h_out, ct_out,
    xg, meta, acc, wbuf, z, pm, stage, ctst, xsem, wsem, osem, csem, send, recv,
):
    pieces, width, tokens, ff, own, ring = dims
    me, xn, yn, pn = neighbours()
    dn = xn + yn - me
    others = [xn, yn, dn] + [device + pn - me for device in (me, xn, yn, dn)]
    total = pieces * own

    def copies(ref, piece, rows, kinds):
        mid = rows // 2
        low, high = pl.ds(0, mid), pl.ds(mid, mid)
        plan = (
            (ref(0).at[low], ref(1).at[low], xn), (ref(0).at[high], ref(1).at[high], xn),
            (ref(0).at[high], ref(2).at[high], yn), (ref(0).at[low], ref(2).at[low], yn), (ref(0), ref(4), pn),
            (ref(1).at[low], ref(3).at[low], yn), (ref(2).at[high], ref(3).at[high], xn),
            (ref(1), ref(5), pn), (ref(2), ref(6), pn), (ref(3), ref(7), pn),
        )
        return [
            pltpu.make_async_remote_copy(
                src_ref=src, dst_ref=dst, send_sem=send.at[piece, kind], recv_sem=recv.at[piece, kind],
                device_id={"ep": device}, device_id_type=MESH,
            )
            for kind, (src, dst, device) in enumerate(plan) if kind in kinds
        ]

    def of_x(c, kinds):
        return copies(lambda q: xg.at[c, q], c, tokens, kinds)

    def of_meta():
        return [
            pltpu.make_async_remote_copy(
                src_ref=meta.at[0], dst_ref=meta.at[q + 1], send_sem=send.at[pieces, q], recv_sem=recv.at[pieces, q],
                device_id={"ep": device}, device_id_type=MESH,
            )
            for q, device in enumerate(others)
        ]

    def start(group):
        for copy in group:
            copy.start()

    def await_recv(group):
        for copy in group:
            copy.wait_recv()

    def load_x(c):
        return pltpu.make_async_copy(x_hbm.at[:, pl.ds(c * width, width)], xg.at[c, 0], xsem.at[c])

    load_meta = pltpu.make_async_copy(meta_hbm, meta.at[0], xsem.at[pieces])

    def w_copy(src, slot, part):
        return pltpu.make_async_copy(src, wbuf.at[slot, :, pl.ds(part * ff, ff)], wsem.at[slot, part])

    def fetch(g):
        slot = lax.rem(g, ring)

        @pl.when(g < total)
        def _():
            rows = pl.ds(pl.multiple_of(g // own * width, width), width)
            for part, src in enumerate((wg, wu)):
                w_copy(src.at[lax.rem(g, own), rows], slot, part).start()

    def await_w(slot):
        for part in range(2):
            w_copy(wg.at[0, pl.ds(0, width)], slot, part).wait()

    load_meta.start()
    for c in range(pieces):
        load_x(c).start()
    greet(others)
    load_meta.wait()
    start(of_meta())
    load_x(0).wait()
    start(of_x(0, OWN_A))
    start(of_x(0, OWN_B))
    for g in range(ring - GROUP):
        fetch(jnp.int32(g))
    for c in range(1, pieces):
        load_x(c).wait()

    def take(group):
        for i in range(GROUP):
            fetch(group * GROUP + ring - GROUP + i)
        slots = [lax.rem(group * GROUP + i, ring) for i in range(GROUP)]
        for slot in slots:
            await_w(slot)
        return slots

    def relay(c):
        await_recv(of_x(c, NEAR_A))
        start(of_x(c, RELAY))

        @pl.when(c + 1 < pieces)
        def _():
            start(of_x(c + 1, OWN_B))

        @pl.when(c + 2 < pieces)
        def _():
            start(of_x(c + 2, OWN_A))

    await_recv(of_x(0, NEAR_A))
    start(of_x(0, RELAY))
    start(of_x(1, OWN_A))
    start(of_x(1, OWN_B))
    start(of_x(2, OWN_A))

    await_recv(of_meta())
    base = (me * (own * PAD)).astype(F32)
    row = lax.broadcasted_iota(jnp.int32, (PAD, tokens), 0).astype(F32)

    def out_ct(q):
        return pltpu.make_async_copy(ctst.at[lax.rem(q, 2)], ct_out.at[q], csem.at[lax.rem(q, 2)])

    def one_hot(q, _):
        @pl.when(q >= 2)
        def _():
            out_ct(q - 2).wait()

        place, gate = meta[q, 0:8] - base, meta[q, 8:16]
        for e in range(own):
            p = jnp.zeros((PAD, tokens), F32)
            c = jnp.zeros((PAD, tokens), F32)
            for j in range(6):
                hit = (place[j : j + 1] - float(e * PAD)) == row
                p = jnp.where(hit, 1.0, p)
                c = jnp.where(hit, gate[j : j + 1], c)
            pm[q, e * PAD : (e + 1) * PAD] = p.astype(BF16)
            ctst[lax.rem(q, 2), e * PAD : (e + 1) * PAD] = c.astype(BF16)
        out_ct(q).start()
        return 0

    lax.fori_loop(0, 8, one_hot, 0)
    for q in (6, 7):
        out_ct(jnp.int32(q)).wait()

    def gather(c):
        def place_rows(q):
            rows = dot(pm[q], xg[c, q]).astype(BF16)
            for e in range(own):
                z[e, q * PAD : (q + 1) * PAD] = rows[e * PAD : (e + 1) * PAD]

        await_recv(of_x(c, PARTNER))
        for q in range(8):
            place_rows(q)

    def pass_on(c):
        @pl.when(c + 1 < pieces)
        def _():
            relay(c + 1)

        await_recv(of_x(c, NEAR_B))
        start(of_x(c, FORWARD))
        await_recv(of_x(c, FAR))
        start(of_x(c, LAST))

    def piece(c, _, new):
        def experts(i, _):
            @pl.when(i == 1)
            def _():
                pass_on(c + 1)

            slots = take(c * own // GROUP + i)
            for j, slot in enumerate(slots):
                e = i * GROUP + j
                lhs = z[e]
                for n0, n1 in spread(2 * ff):
                    term = dot(lhs, wbuf[slot, :, n0:n1])
                    acc[e, :, n0:n1] = term if new else acc[e, :, n0:n1] + term
            return 0

        lax.fori_loop(0, own // GROUP, experts, 0)
        gather(c + 1)
        return 0

    pass_on(jnp.int32(0))
    gather(0)
    piece(jnp.int32(0), 0, True)
    lax.fori_loop(1, pieces - 1, functools.partial(piece, new=False), 0)

    last = pieces - 1

    def out_h(e):
        return pltpu.make_async_copy(stage.at[lax.rem(e, 2)], h_out.at[e], osem.at[lax.rem(e, 2)])

    def finish(i, _):
        slots = take(last * own // GROUP + i)
        for j, slot in enumerate(slots):
            e = i * GROUP + j
            if j >= 2:
                out_h(e - 2).wait()
            else:

                @pl.when(i > 0)
                def _():
                    out_h(e - 2).wait()

            lhs = z[e]
            for n0, n1 in spread(ff):
                a = acc[e, :, n0:n1] + dot(lhs, wbuf[slot, :, n0:n1])
                b = acc[e, :, ff + n0 : ff + n1] + dot(lhs, wbuf[slot, :, ff + n0 : ff + n1])
                stage[j % 2, :, n0:n1] = (jax.nn.silu(a) * b).astype(BF16)
            out_h(e).start()
        return 0

    lax.fori_loop(0, own // GROUP, finish, 0)
    for e in (own - 2, own - 1):
        out_h(jnp.int32(e)).wait()

    def drain(c, _):
        for copy in of_x(c, range(10)):
            copy.wait_send()
        return 0

    lax.fori_loop(0, pieces, drain, 0)
    for copy in of_meta():
        copy.wait_send()


def second_kernel(
    dims, h_hbm, ct_hbm, x_hbm, wd, sg, su, sd, y_hbm,
    h, ct, x, hs, wbuf, ubuf, sbuf, out, keep, dsend, drecv, s1, r1, s2, r2, yst,
    lsem, wsem, usem, ssem, ysem, send, recv,
):
    tiles, width, tokens, own, ring = dims
    me, xn, yn, pn = neighbours()
    half = tokens // 2
    low, high = pl.ds(0, half), pl.ds(half, half)
    slices = hs.shape[1] // width

    def remote(t, kind, src, dst, device):
        return pltpu.make_async_remote_copy(
            src_ref=src, dst_ref=dst, send_sem=send.at[t, kind], recv_sem=recv.at[t, kind],
            device_id={"ep": device}, device_id_type=MESH,
        )

    def to_partner(t):
        return remote(t, 0, dsend.at[lax.rem(t, 3)], drecv.at[t], pn)

    def phase_one(t):
        a, b = pl.ds(0, 2), pl.ds(2, 2)
        return (
            remote(t, 1, s1.at[t, a], r1.at[t, a], xn),
            remote(t, 2, s1.at[t, b], r1.at[t, b], yn),
        )

    def phase_two(t):
        return (
            remote(t, 3, s2.at[t, 0], r2.at[t, 0], yn),
            remote(t, 4, s2.at[t, 1], r2.at[t, 1], xn),
        )

    def columns(t):
        return pl.ds(pl.multiple_of(t * width, width), width)

    def w_copy(g):
        slot = lax.rem(g, ring)
        return pltpu.make_async_copy(wd.at[lax.rem(g, own), :, columns(g // own)], wbuf.at[slot], wsem.at[slot])

    def s_copy(t):
        slot = lax.rem(t, 2)
        return pltpu.make_async_copy(sd.at[:, columns(t)], sbuf.at[slot], ssem.at[slot])

    def u_copies(j):
        slot = lax.rem(j, 2)
        return [
            pltpu.make_async_copy(src.at[:, columns(j)], ubuf.at[slot, part], usem.at[slot, part])
            for part, src in enumerate((sg, su))
        ]

    def h_copy(e):
        return pltpu.make_async_copy(h_hbm.at[e], h.at[e], lsem.at[e])

    def y_copy(t):
        slot = lax.rem(t, 2)
        return pltpu.make_async_copy(yst.at[slot], y_hbm.at[:, columns(t)], ysem.at[slot])

    load_ct = pltpu.make_async_copy(ct_hbm, ct, lsem.at[own])
    load_x = pltpu.make_async_copy(x_hbm, x, lsem.at[own + 1])

    for e in range(own):
        h_copy(e).start()
        if e < ring - BATCH:
            w_copy(jnp.int32(e)).start()
    load_ct.start()
    greet((xn, yn, pn))

    def compute(t):
        def experts(i, _):
            @pl.when(jnp.logical_and(i == 1, t >= 1))
            def _():
                stage_one(t - 1)

            g = t * own + i * BATCH

            @pl.when(g + ring - BATCH < tiles * own)
            def _():
                for j in range(BATCH):
                    w_copy(g + ring - BATCH + j).start()

            @pl.when(t == 0)
            def _():
                for j in range(BATCH):
                    h_copy(i * BATCH + j).wait()

            for j in range(BATCH):
                w_copy(g + j).wait()
            for j in range(BATCH):
                e = i * BATCH + j
                rows = dot(h[e], wbuf[lax.rem(g + j, ring)]).astype(BF16)
                at = pl.ds(pl.multiple_of(e * PAD, 16), PAD)
                for q in range(8):
                    out[q, at] = rows[q * PAD : (q + 1) * PAD]
            return 0

        lax.fori_loop(0, own // BATCH, experts, 0)

        @pl.when(t >= 2)
        def _():
            stage_two(t - 2)

        @pl.when(t == 0)
        def _():
            load_x.start()
            for j in range(2):
                for copy in u_copies(jnp.int32(j)):
                    copy.start()
                s_copy(jnp.int32(j)).start()
            load_ct.wait()

        def terms(q):
            return lax.dot_general(ct[q], out[q], (((0,), (0,)), ((), ())), preferred_element_type=F32)

        @pl.when(t >= 3)
        def _():
            to_partner(t - 3).wait_send()

        for q in range(4, 8):
            dsend[lax.rem(t, 3), q - 4] = terms(q).astype(BF16)
        to_partner(t).start()
        for q in range(4):
            keep[t, q] = terms(q)

    def shared_up(j):
        for copy in u_copies(j):
            copy.wait()
        slot = lax.rem(j, 2)
        a, b = (dot(x[...], ubuf[slot, part]) for part in range(2))
        hs[:, columns(j)] = (jax.nn.silu(a) * b).astype(BF16)

        @pl.when(j + 2 < slices)
        def _():
            for copy in u_copies(j + 2):
                copy.start()

    def shared_down(t):
        s_copy(t).wait()
        keep[t, 0] = keep[t, 0] + dot(hs[...], sbuf[lax.rem(t, 2)])

        @pl.when(t + 2 < tiles)
        def _():
            s_copy(t + 2).start()

    def stage_one(t):
        to_partner(t).wait_recv()

        def both(q, rows):
            return keep[t, q, rows] + drecv[t, q, rows].astype(F32)

        s1[t, 0] = both(1, low).astype(BF16)
        s1[t, 1] = both(3, low).astype(BF16)
        s1[t, 2] = both(2, high).astype(BF16)
        s1[t, 3] = both(3, high).astype(BF16)
        for copy in phase_one(t):
            copy.start()
        keep[t, 0] = keep[t, 0] + drecv[t, 0].astype(F32)
        keep[t, 1, high] = both(1, high)
        keep[t, 2, low] = both(2, low)

    def stage_two(t):
        for copy in phase_one(t):
            copy.wait_recv()
        s2[t, 0] = (keep[t, 2, low] + r1[t, 1].astype(F32)).astype(BF16)
        s2[t, 1] = (keep[t, 1, high] + r1[t, 3].astype(F32)).astype(BF16)
        for copy in phase_two(t):
            copy.start()
        keep[t, 0, low] = keep[t, 0, low] + r1[t, 0].astype(F32)
        keep[t, 0, high] = keep[t, 0, high] + r1[t, 2].astype(F32)

    def stage_three(t):
        for copy in phase_two(t):
            copy.wait_recv()

        @pl.when(t >= 2)
        def _():
            y_copy(t - 2).wait()

        slot = lax.rem(t, 2)
        yst[slot, low] = (keep[t, 0, low] + r2[t, 0].astype(F32)).astype(BF16)
        yst[slot, high] = (keep[t, 0, high] + r2[t, 1].astype(F32)).astype(BF16)
        y_copy(t).start()

    def tile(t, _):
        @pl.when(t < tiles)
        def _():
            compute(t)

        @pl.when(t == 1)
        def _():
            load_x.wait()

        @pl.when(jnp.logical_and(t >= 1, t < tiles - 1))
        def _():
            for i in range(2):

                @pl.when(2 * t - 2 + i < slices)
                def _():
                    shared_up(2 * t - 2 + i)

        @pl.when(t == tiles)
        def _():
            stage_one(t - 1)

        late = 2 * (t - (tiles - 1))

        @pl.when(late >= 0)
        def _():
            shared_down(late)
            shared_down(late + 1)

        @pl.when(jnp.logical_and(t >= tiles, t <= tiles + 1))
        def _():
            stage_two(t - 2)

        @pl.when(late >= 0)
        def _():
            stage_three(late)
            stage_three(late + 1)

        return 0

    lax.fori_loop(0, tiles + 3, tile, 0)
    for t in (tiles - 2, tiles - 1):
        y_copy(jnp.int32(t)).wait()

    def drain(t, _):
        for copy in (*phase_one(t), *phase_two(t)):
            copy.wait_send()
        return 0

    for t in range(tiles - 3, tiles):
        to_partner(jnp.int32(t)).wait_send()

    lax.fori_loop(0, tiles, drain, 0)


def solution(mesh):
    members = mesh.shape["ep"]

    def body(x, expert, slot, gate, w_gate, w_up, w_down, s_gate, s_up, s_down):
        tokens, top = expert.shape[2:]
        own, d, ff = w_gate.shape
        slots = 5 * tokens * top // (4 * own * members)
        x, expert, slot, gate = x[0, 0], expert[0, 0], slot[0, 0], gate[0, 0]
        place = jnp.where(slot < slots, expert * PAD + slot, -1).astype(F32)
        fill = ((0, 8 - top), (0, 0))
        meta = jnp.concatenate([jnp.pad(place.T, fill, constant_values=-1.0), jnp.pad(gate.T, fill)])

        hbm = pl.BlockSpec(memory_space=pl.ANY)
        dma = pltpu.SemaphoreType.DMA
        pieces, ring = 8, 8
        width = d // pieces
        rows = own * PAD
        h, ct = pl.pallas_call(
            functools.partial(first_kernel, (pieces, width, tokens, ff, own, ring)),
            out_shape=(
                jax.ShapeDtypeStruct((own, rows, ff), BF16),
                jax.ShapeDtypeStruct((8, rows, tokens), BF16),
            ),
            in_specs=[hbm] * 4,
            out_specs=(hbm,) * 2,
            scratch_shapes=[
                pltpu.VMEM((pieces, 8, tokens, width), BF16),
                pltpu.VMEM((8, 16, tokens), F32),
                pltpu.VMEM((own, rows, 2 * ff), F32),
                pltpu.VMEM((ring, width, 2 * ff), BF16),
                pltpu.VMEM((own, rows, width), BF16),
                pltpu.VMEM((8, rows, tokens), BF16),
                pltpu.VMEM((2, rows, ff), BF16),
                pltpu.VMEM((2, rows, tokens), BF16),
                dma((pieces + 1,)),
                dma((ring, 2)),
                dma((2,)),
                dma((2,)),
                dma((pieces + 1, 10)),
                dma((pieces + 1, 10)),
            ],
            compiler_params=pltpu.CompilerParams(
                collective_id=0, has_side_effects=True, vmem_limit_bytes=VMEM_BYTES
            ),
            name="dispatch_up",
        )(x, meta, w_gate, w_up)

        tiles, ring = 8, 12
        width = d // tiles
        y = pl.pallas_call(
            functools.partial(second_kernel, (tiles, width, tokens, own, ring)),
            out_shape=jax.ShapeDtypeStruct((tokens, d), BF16),
            in_specs=[hbm] * 7,
            out_specs=hbm,
            scratch_shapes=[
                pltpu.VMEM((own, rows, ff), BF16),
                pltpu.VMEM((8, rows, tokens), BF16),
                pltpu.VMEM((tokens, d), BF16),
                pltpu.VMEM((tokens, 2 * ff), BF16),
                pltpu.VMEM((ring, ff, width), BF16),
                pltpu.VMEM((2, 2, d, width), BF16),
                pltpu.VMEM((2, 2 * ff, width), BF16),
                pltpu.VMEM((8, rows, width), BF16),
                pltpu.VMEM((tiles, 4, tokens, width), F32),
                pltpu.VMEM((3, 4, tokens, width), BF16),
                pltpu.VMEM((tiles, 4, tokens, width), BF16),
                pltpu.VMEM((tiles, 4, tokens // 2, width), BF16),
                pltpu.VMEM((tiles, 4, tokens // 2, width), BF16),
                pltpu.VMEM((tiles, 2, tokens // 2, width), BF16),
                pltpu.VMEM((tiles, 2, tokens // 2, width), BF16),
                pltpu.VMEM((2, tokens, width), BF16),
                dma((own + 2,)),
                dma((ring,)),
                dma((2, 2)),
                dma((2,)),
                dma((2,)),
                dma((tiles, 5)),
                dma((tiles, 5)),
            ],
            compiler_params=pltpu.CompilerParams(
                collective_id=1, has_side_effects=True, vmem_limit_bytes=VMEM_BYTES
            ),
            name="down_combine",
        )(h, ct, x, w_down, s_gate, s_up, s_down)
        return y[None, None]

    tok, exp, rep = P("dp", "ep"), P("ep"), P()
    return jax.shard_map(
        body,
        mesh=mesh,
        in_specs=(tok,) * 4 + (exp,) * 3 + (rep,) * 3,
        out_specs=tok,
        check_vma=False,
    )
```

```python
import functools

import jax
import jax.numpy as jnp
from jax import lax
from jax.experimental import pallas as pl
from jax.experimental.pallas import tpu as pltpu
from jax.sharding import PartitionSpec as P

MESH = pl.DeviceIdType.MESH
F32, BF16 = jnp.float32, jnp.bfloat16
VMEM_BYTES = 67043328
GROUP, BATCH = 4, 4
PAD = 48
OWN_A, OWN_B, RELAY, FORWARD, LAST, PARTNER = (0, 2, 4), (1, 3), (5, 6), (7, 8), (9,), (4, 7, 8, 9)
NEAR_A, NEAR_B, FAR = (0, 2), (1, 3), (5, 6)


def neighbours():
    me = lax.axis_index("ep")
    core, y, x = lax.rem(me, 2), lax.rem(me // 2, 2), me // 4
    return me, me + 4 - 8 * x, me + 2 - 4 * y, me + 1 - 2 * core


def greet(devices, meanwhile=lambda: None):
    barrier = pltpu.get_barrier_semaphore()
    for device in devices:
        pl.semaphore_signal(barrier, inc=1, device_id={"ep": device}, device_id_type=MESH)
    meanwhile()
    pl.semaphore_wait(barrier, len(devices))


def dot(a, b):
    return jnp.dot(a, b, preferred_element_type=F32)


def spread(width):
    return [(n, min(n + 256, width)) for n in range(0, width, 256)]


def first_kernel(
    dims, x_hbm, expert_hbm, slot_hbm, gate_hbm, wg, wu, h_out, ct_out,
    xg, ids, gates, meta, acc, wbuf, z, pm, stage, ctst, xsem, wsem, osem, csem, send, recv,
):
    pieces, width, tokens, ff, own, ring, slots_each, top = dims
    me, xn, yn, pn = neighbours()
    dn = xn + yn - me
    others = [xn, yn, dn] + [device + pn - me for device in (me, xn, yn, dn)]
    total = pieces * own

    def copies(ref, piece, rows, kinds):
        mid = rows // 2
        low, high = pl.ds(0, mid), pl.ds(mid, mid)
        plan = (
            (ref(0).at[low], ref(1).at[low], xn), (ref(0).at[high], ref(1).at[high], xn),
            (ref(0).at[high], ref(2).at[high], yn), (ref(0).at[low], ref(2).at[low], yn), (ref(0), ref(4), pn),
            (ref(1).at[low], ref(3).at[low], yn), (ref(2).at[high], ref(3).at[high], xn),
            (ref(1), ref(5), pn), (ref(2), ref(6), pn), (ref(3), ref(7), pn),
        )
        return [
            pltpu.make_async_remote_copy(
                src_ref=src, dst_ref=dst, send_sem=send.at[piece, kind], recv_sem=recv.at[piece, kind],
                device_id={"ep": device}, device_id_type=MESH,
            )
            for kind, (src, dst, device) in enumerate(plan) if kind in kinds
        ]

    def of_x(c, kinds):
        return copies(lambda q: xg.at[c, q], c, tokens, kinds)

    def of_meta():
        return [
            pltpu.make_async_remote_copy(
                src_ref=meta.at[0], dst_ref=meta.at[q + 1], send_sem=send.at[pieces, q], recv_sem=recv.at[pieces, q],
                device_id={"ep": device}, device_id_type=MESH,
            )
            for q, device in enumerate(others)
        ]

    def start(group):
        for copy in group:
            copy.start()

    def await_recv(group):
        for copy in group:
            copy.wait_recv()

    def load_x(c):
        return pltpu.make_async_copy(x_hbm.at[:, pl.ds(c * width, width)], xg.at[c, 0], xsem.at[c])

    load_meta = [
        pltpu.make_async_copy(src, dst, xsem.at[pieces + i])
        for i, (src, dst) in enumerate(((expert_hbm, ids.at[0]), (slot_hbm, ids.at[1]), (gate_hbm, gates)))
    ]

    def w_copy(src, slot, part):
        return pltpu.make_async_copy(src, wbuf.at[slot, :, pl.ds(part * ff, ff)], wsem.at[slot, part])

    def fetch(g):
        slot = lax.rem(g, ring)

        @pl.when(g < total)
        def _():
            rows = pl.ds(pl.multiple_of(g // own * width, width), width)
            for part, src in enumerate((wg, wu)):
                w_copy(src.at[lax.rem(g, own), rows], slot, part).start()

    def await_w(slot):
        for part in range(2):
            w_copy(wg.at[0, pl.ds(0, width)], slot, part).wait()

    start(load_meta)
    for c in range(pieces):
        load_x(c).start()
    def fill_meta():
        meta[0] = jnp.zeros((16, tokens), F32)
        for copy in load_meta:
            copy.wait()
        for j in range(top):
            slot = ids[1, j]
            place = jnp.where(slot < slots_each, ids[0, j] * PAD + slot, -1)
            meta[0, j : j + 1] = place.astype(F32)
            meta[0, 8 + j : 9 + j] = gates[j]

    greet(others, fill_meta)
    start(of_meta())
    load_x(0).wait()
    start(of_x(0, OWN_A))
    start(of_x(0, OWN_B))
    for g in range(ring - GROUP):
        fetch(jnp.int32(g))
    for c in range(1, pieces):
        load_x(c).wait()

    def take(group):
        for i in range(GROUP):
            fetch(group * GROUP + ring - GROUP + i)
        slots = [lax.rem(group * GROUP + i, ring) for i in range(GROUP)]
        for slot in slots:
            await_w(slot)
        return slots

    def relay(c):
        await_recv(of_x(c, NEAR_A))
        start(of_x(c, RELAY))

        @pl.when(c + 1 < pieces)
        def _():
            start(of_x(c + 1, OWN_B))

        @pl.when(c + 2 < pieces)
        def _():
            start(of_x(c + 2, OWN_A))

    await_recv(of_x(0, NEAR_A))
    start(of_x(0, RELAY))
    start(of_x(1, OWN_A))
    start(of_x(1, OWN_B))
    start(of_x(2, OWN_A))

    await_recv(of_meta())
    base = (me * (own * PAD)).astype(F32)
    row = lax.broadcasted_iota(jnp.int32, (PAD, tokens), 0).astype(F32)

    def out_ct(q):
        return pltpu.make_async_copy(ctst.at[lax.rem(q, 2)], ct_out.at[q], csem.at[lax.rem(q, 2)])

    def one_hot(q, _):
        @pl.when(q >= 2)
        def _():
            out_ct(q - 2).wait()

        place, gate = meta[q, 0:8] - base, meta[q, 8:16]
        for e in range(own):
            p = jnp.zeros((PAD, tokens), F32)
            c = jnp.zeros((PAD, tokens), F32)
            for j in range(top):
                hit = (place[j : j + 1] - float(e * PAD)) == row
                p = jnp.where(hit, 1.0, p)
                c = jnp.where(hit, gate[j : j + 1], c)
            pm[q, e * PAD : (e + 1) * PAD] = p.astype(BF16)
            ctst[lax.rem(q, 2), e * PAD : (e + 1) * PAD] = c.astype(BF16)
        out_ct(q).start()
        return 0

    lax.fori_loop(0, 8, one_hot, 0)
    for q in (6, 7):
        out_ct(jnp.int32(q)).wait()

    def gather(c):
        def place_rows(q):
            rows = dot(pm[q], xg[c, q]).astype(BF16)
            for e in range(own):
                z[e, q * PAD : (q + 1) * PAD] = rows[e * PAD : (e + 1) * PAD]

        await_recv(of_x(c, PARTNER))
        for q in range(8):
            place_rows(q)

    def pass_on(c):
        @pl.when(c + 1 < pieces)
        def _():
            relay(c + 1)

        await_recv(of_x(c, NEAR_B))
        start(of_x(c, FORWARD))
        await_recv(of_x(c, FAR))
        start(of_x(c, LAST))

    def piece(c, _, new):
        def experts(i, _):
            @pl.when(i == 1)
            def _():
                pass_on(c + 1)

            slots = take(c * own // GROUP + i)
            for j, slot in enumerate(slots):
                e = i * GROUP + j
                lhs = z[e]
                for n0, n1 in spread(2 * ff):
                    term = dot(lhs, wbuf[slot, :, n0:n1])
                    acc[e, :, n0:n1] = term if new else acc[e, :, n0:n1] + term
            return 0

        lax.fori_loop(0, own // GROUP, experts, 0)
        gather(c + 1)
        return 0

    pass_on(jnp.int32(0))
    gather(0)
    piece(jnp.int32(0), 0, True)
    lax.fori_loop(1, pieces - 1, functools.partial(piece, new=False), 0)

    last = pieces - 1

    def out_h(e):
        return pltpu.make_async_copy(stage.at[lax.rem(e, 2)], h_out.at[e], osem.at[lax.rem(e, 2)])

    def finish(i, _):
        slots = take(last * own // GROUP + i)
        for j, slot in enumerate(slots):
            e = i * GROUP + j
            if j >= 2:
                out_h(e - 2).wait()
            else:

                @pl.when(i > 0)
                def _():
                    out_h(e - 2).wait()

            lhs = z[e]
            for n0, n1 in spread(ff):
                a = acc[e, :, n0:n1] + dot(lhs, wbuf[slot, :, n0:n1])
                b = acc[e, :, ff + n0 : ff + n1] + dot(lhs, wbuf[slot, :, ff + n0 : ff + n1])
                stage[j % 2, :, n0:n1] = (jax.nn.silu(a) * b).astype(BF16)
            out_h(e).start()
        return 0

    lax.fori_loop(0, own // GROUP, finish, 0)
    for e in (own - 2, own - 1):
        out_h(jnp.int32(e)).wait()

    def drain(c, _):
        for copy in of_x(c, range(10)):
            copy.wait_send()
        return 0

    lax.fori_loop(0, pieces, drain, 0)
    for copy in of_meta():
        copy.wait_send()


def second_kernel(
    dims, h_hbm, ct_hbm, x_hbm, wd, sg, su, sd, y_hbm,
    h, ct, x, hs, wbuf, ubuf, sbuf, out, keep, dsend, drecv, s1, r1, s2, r2, yst,
    lsem, wsem, usem, ssem, ysem, send, recv,
):
    tiles, width, tokens, own, ring = dims
    me, xn, yn, pn = neighbours()
    half = tokens // 2
    low, high = pl.ds(0, half), pl.ds(half, half)
    slices = hs.shape[1] // width

    def remote(t, kind, src, dst, device):
        return pltpu.make_async_remote_copy(
            src_ref=src, dst_ref=dst, send_sem=send.at[t, kind], recv_sem=recv.at[t, kind],
            device_id={"ep": device}, device_id_type=MESH,
        )

    def to_partner(t):
        return remote(t, 0, dsend.at[lax.rem(t, 3)], drecv.at[t], pn)

    def phase_one(t):
        a, b = pl.ds(0, 2), pl.ds(2, 2)
        return (
            remote(t, 1, s1.at[t, a], r1.at[t, a], xn),
            remote(t, 2, s1.at[t, b], r1.at[t, b], yn),
        )

    def phase_two(t):
        return (
            remote(t, 3, s2.at[t, 0], r2.at[t, 0], yn),
            remote(t, 4, s2.at[t, 1], r2.at[t, 1], xn),
        )

    def columns(t):
        return pl.ds(pl.multiple_of(t * width, width), width)

    def w_copy(g):
        slot = lax.rem(g, ring)
        return pltpu.make_async_copy(wd.at[lax.rem(g, own), :, columns(g // own)], wbuf.at[slot], wsem.at[slot])

    def s_copy(t):
        slot = lax.rem(t, 2)
        return pltpu.make_async_copy(sd.at[:, columns(t)], sbuf.at[slot], ssem.at[slot])

    def u_copies(j):
        slot = lax.rem(j, 2)
        return [
            pltpu.make_async_copy(src.at[:, columns(j)], ubuf.at[slot, part], usem.at[slot, part])
            for part, src in enumerate((sg, su))
        ]

    def h_copy(e):
        return pltpu.make_async_copy(h_hbm.at[e], h.at[e], lsem.at[e])

    def y_copy(t):
        slot = lax.rem(t, 2)
        return pltpu.make_async_copy(yst.at[slot], y_hbm.at[:, columns(t)], ysem.at[slot])

    load_ct = pltpu.make_async_copy(ct_hbm, ct, lsem.at[own])
    load_x = pltpu.make_async_copy(x_hbm, x, lsem.at[own + 1])

    for e in range(own):
        h_copy(e).start()
        if e < ring - BATCH:
            w_copy(jnp.int32(e)).start()
    load_ct.start()
    greet((xn, yn, pn))

    def compute(t):
        def experts(i, _):
            @pl.when(jnp.logical_and(i == 1, t >= 1))
            def _():
                stage_one(t - 1)

            g = t * own + i * BATCH

            @pl.when(g + ring - BATCH < tiles * own)
            def _():
                for j in range(BATCH):
                    w_copy(g + ring - BATCH + j).start()

            @pl.when(t == 0)
            def _():
                for j in range(BATCH):
                    h_copy(i * BATCH + j).wait()

            for j in range(BATCH):
                w_copy(g + j).wait()
            for j in range(BATCH):
                e = i * BATCH + j
                rows = dot(h[e], wbuf[lax.rem(g + j, ring)]).astype(BF16)
                at = pl.ds(pl.multiple_of(e * PAD, 16), PAD)
                for q in range(8):
                    out[q, at] = rows[q * PAD : (q + 1) * PAD]
            return 0

        lax.fori_loop(0, own // BATCH, experts, 0)

        @pl.when(t >= 2)
        def _():
            stage_two(t - 2)

        @pl.when(t == 0)
        def _():
            load_x.start()
            for j in range(2):
                for copy in u_copies(jnp.int32(j)):
                    copy.start()
                s_copy(jnp.int32(j)).start()
            load_ct.wait()

        def terms(q):
            return lax.dot_general(ct[q], out[q], (((0,), (0,)), ((), ())), preferred_element_type=F32)

        @pl.when(t >= 3)
        def _():
            to_partner(t - 3).wait_send()

        for q in range(4, 8):
            dsend[lax.rem(t, 3), q - 4] = terms(q).astype(BF16)
        to_partner(t).start()
        for q in range(4):
            keep[t, q] = terms(q)

    def shared_up(j):
        for copy in u_copies(j):
            copy.wait()
        slot = lax.rem(j, 2)
        a, b = (dot(x[...], ubuf[slot, part]) for part in range(2))
        hs[:, columns(j)] = (jax.nn.silu(a) * b).astype(BF16)

        @pl.when(j + 2 < slices)
        def _():
            for copy in u_copies(j + 2):
                copy.start()

    def shared_down(t):
        s_copy(t).wait()
        keep[t, 0] = keep[t, 0] + dot(hs[...], sbuf[lax.rem(t, 2)])

        @pl.when(t + 2 < tiles)
        def _():
            s_copy(t + 2).start()

    def stage_one(t):
        to_partner(t).wait_recv()

        def both(q, rows):
            return keep[t, q, rows] + drecv[t, q, rows].astype(F32)

        s1[t, 0] = both(1, low).astype(BF16)
        s1[t, 1] = both(3, low).astype(BF16)
        s1[t, 2] = both(2, high).astype(BF16)
        s1[t, 3] = both(3, high).astype(BF16)
        for copy in phase_one(t):
            copy.start()
        keep[t, 0] = keep[t, 0] + drecv[t, 0].astype(F32)
        keep[t, 1, high] = both(1, high)
        keep[t, 2, low] = both(2, low)

    def stage_two(t):
        for copy in phase_one(t):
            copy.wait_recv()
        s2[t, 0] = (keep[t, 2, low] + r1[t, 1].astype(F32)).astype(BF16)
        s2[t, 1] = (keep[t, 1, high] + r1[t, 3].astype(F32)).astype(BF16)
        for copy in phase_two(t):
            copy.start()
        keep[t, 0, low] = keep[t, 0, low] + r1[t, 0].astype(F32)
        keep[t, 0, high] = keep[t, 0, high] + r1[t, 2].astype(F32)

    def stage_three(t):
        for copy in phase_two(t):
            copy.wait_recv()

        @pl.when(t >= 2)
        def _():
            y_copy(t - 2).wait()

        slot = lax.rem(t, 2)
        yst[slot, low] = (keep[t, 0, low] + r2[t, 0].astype(F32)).astype(BF16)
        yst[slot, high] = (keep[t, 0, high] + r2[t, 1].astype(F32)).astype(BF16)
        y_copy(t).start()

    def tile(t, _):
        @pl.when(t < tiles)
        def _():
            compute(t)

        @pl.when(t == 1)
        def _():
            load_x.wait()

        @pl.when(jnp.logical_and(t >= 1, t < tiles - 1))
        def _():
            for i in range(2):

                @pl.when(2 * t - 2 + i < slices)
                def _():
                    shared_up(2 * t - 2 + i)

        @pl.when(t == tiles)
        def _():
            stage_one(t - 1)

        late = 2 * (t - (tiles - 1))

        @pl.when(late >= 0)
        def _():
            shared_down(late)
            shared_down(late + 1)

        @pl.when(jnp.logical_and(t >= tiles, t <= tiles + 1))
        def _():
            stage_two(t - 2)

        @pl.when(late >= 0)
        def _():
            stage_three(late)
            stage_three(late + 1)

        return 0

    lax.fori_loop(0, tiles + 3, tile, 0)
    for t in (tiles - 2, tiles - 1):
        y_copy(jnp.int32(t)).wait()

    def drain(t, _):
        for copy in (*phase_one(t), *phase_two(t)):
            copy.wait_send()
        return 0

    for t in range(tiles - 3, tiles):
        to_partner(jnp.int32(t)).wait_send()

    lax.fori_loop(0, tiles, drain, 0)


def solution(mesh):
    members = mesh.shape["ep"]

    def body(x, expert, slot, gate, w_gate, w_up, w_down, s_gate, s_up, s_down):
        tokens, top = expert.shape[2:]
        own, d, ff = w_gate.shape
        slots = 5 * tokens * top // (4 * own * members)
        x = x[0, 0]
        expert, slot, gate = (v.transpose(3, 0, 1, 2).reshape(top, 1, tokens) for v in (expert, slot, gate))

        hbm = pl.BlockSpec(memory_space=pl.ANY)
        dma = pltpu.SemaphoreType.DMA
        pieces, ring = 8, 8
        width = d // pieces
        rows = own * PAD
        h, ct = pl.pallas_call(
            functools.partial(first_kernel, (pieces, width, tokens, ff, own, ring, slots, top)),
            out_shape=(
                jax.ShapeDtypeStruct((own, rows, ff), BF16),
                jax.ShapeDtypeStruct((8, rows, tokens), BF16),
            ),
            in_specs=[hbm] * 6,
            out_specs=(hbm,) * 2,
            scratch_shapes=[
                pltpu.VMEM((pieces, 8, tokens, width), BF16),
                pltpu.VMEM((2, top, 1, tokens), jnp.int32),
                pltpu.VMEM((top, 1, tokens), F32),
                pltpu.VMEM((8, 16, tokens), F32),
                pltpu.VMEM((own, rows, 2 * ff), F32),
                pltpu.VMEM((ring, width, 2 * ff), BF16),
                pltpu.VMEM((own, rows, width), BF16),
                pltpu.VMEM((8, rows, tokens), BF16),
                pltpu.VMEM((2, rows, ff), BF16),
                pltpu.VMEM((2, rows, tokens), BF16),
                dma((pieces + 3,)),
                dma((ring, 2)),
                dma((2,)),
                dma((2,)),
                dma((pieces + 1, 10)),
                dma((pieces + 1, 10)),
            ],
            compiler_params=pltpu.CompilerParams(
                collective_id=0, has_side_effects=True, vmem_limit_bytes=VMEM_BYTES
            ),
            name="dispatch_up",
        )(x, expert, slot, gate, w_gate, w_up)

        tiles, ring = 8, 12
        width = d // tiles
        y = pl.pallas_call(
            functools.partial(second_kernel, (tiles, width, tokens, own, ring)),
            out_shape=jax.ShapeDtypeStruct((tokens, d), BF16),
            in_specs=[hbm] * 7,
            out_specs=hbm,
            scratch_shapes=[
                pltpu.VMEM((own, rows, ff), BF16),
                pltpu.VMEM((8, rows, tokens), BF16),
                pltpu.VMEM((tokens, d), BF16),
                pltpu.VMEM((tokens, 2 * ff), BF16),
                pltpu.VMEM((ring, ff, width), BF16),
                pltpu.VMEM((2, 2, d, width), BF16),
                pltpu.VMEM((2, 2 * ff, width), BF16),
                pltpu.VMEM((8, rows, width), BF16),
                pltpu.VMEM((tiles, 4, tokens, width), F32),
                pltpu.VMEM((3, 4, tokens, width), BF16),
                pltpu.VMEM((tiles, 4, tokens, width), BF16),
                pltpu.VMEM((tiles, 4, tokens // 2, width), BF16),
                pltpu.VMEM((tiles, 4, tokens // 2, width), BF16),
                pltpu.VMEM((tiles, 2, tokens // 2, width), BF16),
                pltpu.VMEM((tiles, 2, tokens // 2, width), BF16),
                pltpu.VMEM((2, tokens, width), BF16),
                dma((own + 2,)),
                dma((ring,)),
                dma((2, 2)),
                dma((2,)),
                dma((2,)),
                dma((tiles, 5)),
                dma((tiles, 5)),
            ],
            compiler_params=pltpu.CompilerParams(
                collective_id=1, has_side_effects=True, vmem_limit_bytes=VMEM_BYTES
            ),
            name="down_combine",
        )(h, ct, x, w_down, s_gate, s_up, s_down)
        return y[None, None]

    tok, exp, rep = P("dp", "ep"), P("ep"), P()
    return jax.shard_map(
        body,
        mesh=mesh,
        in_specs=(tok,) * 4 + (exp,) * 3 + (rep,) * 3,
        out_specs=tok,
        check_vma=False,
    )
```

```python
import functools

import jax
import jax.numpy as jnp
from jax import lax
from jax.experimental import pallas as pl
from jax.experimental.pallas import tpu as pltpu
from jax.sharding import PartitionSpec as P

MESH = pl.DeviceIdType.MESH
F32, BF16 = jnp.float32, jnp.bfloat16
VMEM_BYTES = 67043328
GROUP, BATCH = 4, 4
PAD = 48
OWN_A, OWN_B, RELAY, FORWARD, LAST, PARTNER = (0, 2, 4), (1, 3), (5, 6), (7, 8), (9,), (4, 7, 8, 9)
NEAR_A, NEAR_B, FAR = (0, 2), (1, 3), (5, 6)


def neighbours():
    me = lax.axis_index("ep")
    core, y, x = lax.rem(me, 2), lax.rem(me // 2, 2), me // 4
    return me, me + 4 - 8 * x, me + 2 - 4 * y, me + 1 - 2 * core


def greet(devices, meanwhile=lambda: None):
    barrier = pltpu.get_barrier_semaphore()
    for device in devices:
        pl.semaphore_signal(barrier, inc=1, device_id={"ep": device}, device_id_type=MESH)
    meanwhile()
    pl.semaphore_wait(barrier, len(devices))


def dot(a, b):
    return jnp.dot(a, b, preferred_element_type=F32)


def spread(width):
    return [(n, min(n + 256, width)) for n in range(0, width, 256)]


def first_kernel(
    dims, x_hbm, expert_hbm, slot_hbm, gate_hbm, wg, wu, h_out, ct_out,
    xg, ids, gates, meta, acc, wbuf, z, pm, stage, ctst, xsem, wsem, osem, csem, send, recv,
):
    pieces, width, tokens, ff, own, ring, slots_each, top = dims
    me, xn, yn, pn = neighbours()
    dn = xn + yn - me
    others = [xn, yn, dn] + [device + pn - me for device in (me, xn, yn, dn)]
    total = pieces * own

    def copies(ref, piece, rows, kinds):
        mid = rows // 2
        low, high = pl.ds(0, mid), pl.ds(mid, mid)
        plan = (
            (ref(0).at[low], ref(1).at[low], xn), (ref(0).at[high], ref(1).at[high], xn),
            (ref(0).at[high], ref(2).at[high], yn), (ref(0).at[low], ref(2).at[low], yn), (ref(0), ref(4), pn),
            (ref(1).at[low], ref(3).at[low], yn), (ref(2).at[high], ref(3).at[high], xn),
            (ref(1), ref(5), pn), (ref(2), ref(6), pn), (ref(3), ref(7), pn),
        )
        return [
            pltpu.make_async_remote_copy(
                src_ref=src, dst_ref=dst, send_sem=send.at[piece, kind], recv_sem=recv.at[piece, kind],
                device_id={"ep": device}, device_id_type=MESH,
            )
            for kind, (src, dst, device) in enumerate(plan) if kind in kinds
        ]

    def of_x(c, kinds):
        return copies(lambda q: xg.at[c, q], c, tokens, kinds)

    def of_meta():
        return [
            pltpu.make_async_remote_copy(
                src_ref=meta.at[0], dst_ref=meta.at[q + 1], send_sem=send.at[pieces, q], recv_sem=recv.at[pieces, q],
                device_id={"ep": device}, device_id_type=MESH,
            )
            for q, device in enumerate(others)
        ]

    def start(group):
        for copy in group:
            copy.start()

    def await_recv(group):
        for copy in group:
            copy.wait_recv()

    def load_x(c):
        return pltpu.make_async_copy(x_hbm.at[:, pl.ds(c * width, width)], xg.at[c, 0], xsem.at[c])

    load_meta = [
        pltpu.make_async_copy(src, dst, xsem.at[pieces + i])
        for i, (src, dst) in enumerate(((expert_hbm, ids.at[0]), (slot_hbm, ids.at[1]), (gate_hbm, gates)))
    ]

    def w_copy(src, slot, part):
        return pltpu.make_async_copy(src, wbuf.at[slot, :, pl.ds(part * ff, ff)], wsem.at[slot, part])

    def fetch(g):
        slot = lax.rem(g, ring)

        @pl.when(g < total)
        def _():
            rows = pl.ds(pl.multiple_of(g // own * width, width), width)
            for part, src in enumerate((wg, wu)):
                w_copy(src.at[lax.rem(g, own), rows], slot, part).start()

    def await_w(slot):
        for part in range(2):
            w_copy(wg.at[0, pl.ds(0, width)], slot, part).wait()

    start(load_meta)
    for c in range(pieces):
        load_x(c).start()
    def fill_meta():
        meta[0] = jnp.zeros((16, tokens), F32)
        for copy in load_meta:
            copy.wait()
        for j in range(top):
            slot = ids[1, j]
            place = jnp.where(slot < slots_each, ids[0, j] * PAD + slot, -1)
            meta[0, j : j + 1] = place.astype(F32)
            meta[0, 8 + j : 9 + j] = gates[j]

    greet(others, fill_meta)
    start(of_meta())
    load_x(0).wait()
    start(of_x(0, OWN_A))
    start(of_x(0, OWN_B))
    for g in range(ring - GROUP):
        fetch(jnp.int32(g))
    for c in range(1, pieces):
        load_x(c).wait()

    def take(group):
        for i in range(GROUP):
            fetch(group * GROUP + ring - GROUP + i)
        slots = [lax.rem(group * GROUP + i, ring) for i in range(GROUP)]
        for slot in slots:
            await_w(slot)
        return slots

    def relay(c):
        await_recv(of_x(c, NEAR_A))
        start(of_x(c, RELAY))

        @pl.when(c + 1 < pieces)
        def _():
            start(of_x(c + 1, OWN_B))

        @pl.when(c + 2 < pieces)
        def _():
            start(of_x(c + 2, OWN_A))

    await_recv(of_x(0, NEAR_A))
    start(of_x(0, RELAY))
    start(of_x(1, OWN_A))
    start(of_x(1, OWN_B))
    start(of_x(2, OWN_A))

    await_recv(of_meta())
    base = (me * (own * PAD)).astype(F32)
    row = lax.broadcasted_iota(jnp.int32, (PAD, tokens), 0).astype(F32)

    def out_ct(q):
        return pltpu.make_async_copy(ctst.at[lax.rem(q, 2)], ct_out.at[q], csem.at[lax.rem(q, 2)])

    def one_hot(q, _):
        @pl.when(q >= 2)
        def _():
            out_ct(q - 2).wait()

        place, gate = meta[q, 0:8] - base, meta[q, 8:16]
        for e in range(own):
            p = jnp.zeros((PAD, tokens), F32)
            c = jnp.zeros((PAD, tokens), F32)
            for j in range(top):
                hit = (place[j : j + 1] - float(e * PAD)) == row
                p = jnp.where(hit, 1.0, p)
                c = jnp.where(hit, gate[j : j + 1], c)
            pm[q, e * PAD : (e + 1) * PAD] = p.astype(BF16)
            ctst[lax.rem(q, 2), e * PAD : (e + 1) * PAD] = c.astype(BF16)
        out_ct(q).start()
        return 0

    lax.fori_loop(0, 8, one_hot, 0)
    for q in (6, 7):
        out_ct(jnp.int32(q)).wait()

    def gather(c):
        def place_rows(q):
            rows = dot(pm[q], xg[c, q]).astype(BF16)
            for e in range(own):
                z[e, q * PAD : (q + 1) * PAD] = rows[e * PAD : (e + 1) * PAD]

        await_recv(of_x(c, PARTNER))
        for q in range(8):
            place_rows(q)

    def pass_on(c):
        @pl.when(c + 1 < pieces)
        def _():
            relay(c + 1)

        await_recv(of_x(c, NEAR_B))
        start(of_x(c, FORWARD))
        await_recv(of_x(c, FAR))
        start(of_x(c, LAST))

    def piece(c, _, new):
        def experts(i, _):
            @pl.when(i == 1)
            def _():
                pass_on(c + 1)

            slots = take(c * own // GROUP + i)
            for j, slot in enumerate(slots):
                e = i * GROUP + j
                lhs = z[e]
                for n0, n1 in spread(2 * ff):
                    term = dot(lhs, wbuf[slot, :, n0:n1])
                    acc[e, :, n0:n1] = term if new else acc[e, :, n0:n1] + term
            return 0

        lax.fori_loop(0, own // GROUP, experts, 0)
        gather(c + 1)
        return 0

    pass_on(jnp.int32(0))
    gather(0)
    piece(jnp.int32(0), 0, True)
    lax.fori_loop(1, pieces - 1, functools.partial(piece, new=False), 0)

    last = pieces - 1

    def out_h(e):
        return pltpu.make_async_copy(stage.at[lax.rem(e, 2)], h_out.at[e], osem.at[lax.rem(e, 2)])

    def finish(i, _):
        slots = take(last * own // GROUP + i)
        for j, slot in enumerate(slots):
            e = i * GROUP + j
            if j >= 2:
                out_h(e - 2).wait()
            else:

                @pl.when(i > 0)
                def _():
                    out_h(e - 2).wait()

            lhs = z[e]
            for n0, n1 in spread(ff):
                a = acc[e, :, n0:n1] + dot(lhs, wbuf[slot, :, n0:n1])
                b = acc[e, :, ff + n0 : ff + n1] + dot(lhs, wbuf[slot, :, ff + n0 : ff + n1])
                stage[j % 2, :, n0:n1] = (jax.nn.silu(a) * b).astype(BF16)
            out_h(e).start()
        return 0

    lax.fori_loop(0, own // GROUP, finish, 0)
    for e in (own - 2, own - 1):
        out_h(jnp.int32(e)).wait()

    def drain(c, _):
        for copy in of_x(c, range(10)):
            copy.wait_send()
        return 0

    lax.fori_loop(0, pieces, drain, 0)
    for copy in of_meta():
        copy.wait_send()


def second_kernel(
    dims, h_hbm, ct_hbm, x_hbm, wd, sg, su, sd, y_hbm,
    h, ct, x, hs, wbuf, ubuf, sbuf, out, keep, dsend, drecv, s1, r1, s2, r2, yst,
    lsem, wsem, usem, ssem, ysem, send, recv,
):
    tiles, width, tokens, own, ring = dims
    me, xn, yn, pn = neighbours()
    half = tokens // 2
    low, high = pl.ds(0, half), pl.ds(half, half)
    slices = hs.shape[1] // width

    def remote(t, kind, src, dst, device):
        return pltpu.make_async_remote_copy(
            src_ref=src, dst_ref=dst, send_sem=send.at[t, kind], recv_sem=recv.at[t, kind],
            device_id={"ep": device}, device_id_type=MESH,
        )

    def to_partner(t):
        return remote(t, 0, dsend.at[lax.rem(t, 3)], drecv.at[t], pn)

    def phase_one(t):
        return [
            remote(t, kind, s1.at[t, i], r1.at[t, i], device)
            for kind, i, device in ((1, 1, xn), (2, 3, yn), (5, 0, xn), (6, 2, yn))
        ]

    def phase_two(t):
        return (
            remote(t, 3, s2.at[t, 0], r2.at[t, 0], yn),
            remote(t, 4, s2.at[t, 1], r2.at[t, 1], xn),
        )

    def columns(t):
        return pl.ds(pl.multiple_of(t * width, width), width)

    def w_copy(g):
        slot = lax.rem(g, ring)
        return pltpu.make_async_copy(wd.at[lax.rem(g, own), :, columns(g // own)], wbuf.at[slot], wsem.at[slot])

    def s_copy(t):
        slot = lax.rem(t, 2)
        return pltpu.make_async_copy(sd.at[:, columns(t)], sbuf.at[slot], ssem.at[slot])

    def u_copies(j):
        slot = lax.rem(j, 2)
        return [
            pltpu.make_async_copy(src.at[:, columns(j)], ubuf.at[slot, part], usem.at[slot, part])
            for part, src in enumerate((sg, su))
        ]

    def h_copy(e):
        return pltpu.make_async_copy(h_hbm.at[e], h.at[e], lsem.at[e])

    def y_copy(t):
        slot = lax.rem(t, 2)
        return pltpu.make_async_copy(yst.at[slot], y_hbm.at[:, columns(t)], ysem.at[slot])

    load_ct = pltpu.make_async_copy(ct_hbm, ct, lsem.at[own])
    load_x = pltpu.make_async_copy(x_hbm, x, lsem.at[own + 1])

    for e in range(own):
        h_copy(e).start()
        if e < ring - BATCH:
            w_copy(jnp.int32(e)).start()
    load_ct.start()
    greet((xn, yn, pn))

    def compute(t):
        def experts(i, _):
            @pl.when(jnp.logical_and(i == 1, t >= 1))
            def _():
                stage_one(t - 1)

            g = t * own + i * BATCH

            @pl.when(g + ring - BATCH < tiles * own)
            def _():
                for j in range(BATCH):
                    w_copy(g + ring - BATCH + j).start()

            @pl.when(t == 0)
            def _():
                for j in range(BATCH):
                    h_copy(i * BATCH + j).wait()

            for j in range(BATCH):
                w_copy(g + j).wait()
            for j in range(BATCH):
                e = i * BATCH + j
                rows = dot(h[e], wbuf[lax.rem(g + j, ring)]).astype(BF16)
                at = pl.ds(pl.multiple_of(e * PAD, 16), PAD)
                for q in range(8):
                    out[q, at] = rows[q * PAD : (q + 1) * PAD]
            return 0

        lax.fori_loop(0, own // BATCH, experts, 0)

        @pl.when(t >= 2)
        def _():
            stage_two(t - 2)

        @pl.when(t == 0)
        def _():
            load_x.start()
            for j in range(2):
                for copy in u_copies(jnp.int32(j)):
                    copy.start()
                s_copy(jnp.int32(j)).start()
            load_ct.wait()

        def terms(q):
            return lax.dot_general(ct[q], out[q], (((0,), (0,)), ((), ())), preferred_element_type=F32)

        @pl.when(t >= 3)
        def _():
            to_partner(t - 3).wait_send()

        for q in range(4, 8):
            dsend[lax.rem(t, 3), q - 4] = terms(q).astype(BF16)
        to_partner(t).start()
        for q in range(4):
            keep[t, q] = terms(q)

    def shared_up(j):
        for copy in u_copies(j):
            copy.wait()
        slot = lax.rem(j, 2)
        a, b = (dot(x[...], ubuf[slot, part]) for part in range(2))
        hs[:, columns(j)] = (jax.nn.silu(a) * b).astype(BF16)

        @pl.when(j + 2 < slices)
        def _():
            for copy in u_copies(j + 2):
                copy.start()

    def shared_down(t):
        s_copy(t).wait()
        keep[t, 0] = keep[t, 0] + dot(hs[...], sbuf[lax.rem(t, 2)])

        @pl.when(t + 2 < tiles)
        def _():
            s_copy(t + 2).start()

    def stage_one(t):
        to_partner(t).wait_recv()

        def both(q, rows):
            return keep[t, q, rows] + drecv[t, q, rows].astype(F32)

        s1[t, 0] = both(1, low).astype(BF16)
        s1[t, 1] = both(3, low).astype(BF16)
        s1[t, 2] = both(2, high).astype(BF16)
        s1[t, 3] = both(3, high).astype(BF16)
        for copy in phase_one(t):
            copy.start()
        keep[t, 0] = keep[t, 0] + drecv[t, 0].astype(F32)
        keep[t, 1, high] = both(1, high)
        keep[t, 2, low] = both(2, low)

    def stage_two(t):
        arrivals = phase_one(t)
        for copy in arrivals[:2]:
            copy.wait_recv()
        s2[t, 0] = (keep[t, 2, low] + r1[t, 1].astype(F32)).astype(BF16)
        s2[t, 1] = (keep[t, 1, high] + r1[t, 3].astype(F32)).astype(BF16)
        for copy in phase_two(t):
            copy.start()
        for copy in arrivals[2:]:
            copy.wait_recv()
        keep[t, 0, low] = keep[t, 0, low] + r1[t, 0].astype(F32)
        keep[t, 0, high] = keep[t, 0, high] + r1[t, 2].astype(F32)

    def stage_three(t):
        for copy in phase_two(t):
            copy.wait_recv()

        @pl.when(t >= 2)
        def _():
            y_copy(t - 2).wait()

        slot = lax.rem(t, 2)
        yst[slot, low] = (keep[t, 0, low] + r2[t, 0].astype(F32)).astype(BF16)
        yst[slot, high] = (keep[t, 0, high] + r2[t, 1].astype(F32)).astype(BF16)
        y_copy(t).start()

    def tile(t, _):
        @pl.when(t < tiles)
        def _():
            compute(t)

        @pl.when(t == 1)
        def _():
            load_x.wait()

        @pl.when(jnp.logical_and(t >= 1, t < tiles - 1))
        def _():
            for i in range(2):

                @pl.when(2 * t - 2 + i < slices)
                def _():
                    shared_up(2 * t - 2 + i)

        @pl.when(t == tiles)
        def _():
            stage_one(t - 1)

        late = 2 * (t - (tiles - 1))

        @pl.when(late >= 0)
        def _():
            shared_down(late)
            shared_down(late + 1)

        @pl.when(jnp.logical_and(t >= tiles, t <= tiles + 1))
        def _():
            stage_two(t - 2)

        @pl.when(late >= 0)
        def _():
            stage_three(late)
            stage_three(late + 1)

        return 0

    lax.fori_loop(0, tiles + 3, tile, 0)
    for t in (tiles - 2, tiles - 1):
        y_copy(jnp.int32(t)).wait()

    def drain(t, _):
        for copy in (*phase_one(t), *phase_two(t)):
            copy.wait_send()
        return 0

    for t in range(tiles - 3, tiles):
        to_partner(jnp.int32(t)).wait_send()

    lax.fori_loop(0, tiles, drain, 0)


def solution(mesh):
    members = mesh.shape["ep"]

    def body(x, expert, slot, gate, w_gate, w_up, w_down, s_gate, s_up, s_down):
        tokens, top = expert.shape[2:]
        own, d, ff = w_gate.shape
        slots = 5 * tokens * top // (4 * own * members)
        x = x[0, 0]
        expert, slot, gate = (v.transpose(3, 0, 1, 2).reshape(top, 1, tokens) for v in (expert, slot, gate))

        hbm = pl.BlockSpec(memory_space=pl.ANY)
        dma = pltpu.SemaphoreType.DMA
        pieces, ring = 8, 8
        width = d // pieces
        rows = own * PAD
        h, ct = pl.pallas_call(
            functools.partial(first_kernel, (pieces, width, tokens, ff, own, ring, slots, top)),
            out_shape=(
                jax.ShapeDtypeStruct((own, rows, ff), BF16),
                jax.ShapeDtypeStruct((8, rows, tokens), BF16),
            ),
            in_specs=[hbm] * 6,
            out_specs=(hbm,) * 2,
            scratch_shapes=[
                pltpu.VMEM((pieces, 8, tokens, width), BF16),
                pltpu.VMEM((2, top, 1, tokens), jnp.int32),
                pltpu.VMEM((top, 1, tokens), F32),
                pltpu.VMEM((8, 16, tokens), F32),
                pltpu.VMEM((own, rows, 2 * ff), F32),
                pltpu.VMEM((ring, width, 2 * ff), BF16),
                pltpu.VMEM((own, rows, width), BF16),
                pltpu.VMEM((8, rows, tokens), BF16),
                pltpu.VMEM((2, rows, ff), BF16),
                pltpu.VMEM((2, rows, tokens), BF16),
                dma((pieces + 3,)),
                dma((ring, 2)),
                dma((2,)),
                dma((2,)),
                dma((pieces + 1, 10)),
                dma((pieces + 1, 10)),
            ],
            compiler_params=pltpu.CompilerParams(
                collective_id=0, has_side_effects=True, vmem_limit_bytes=VMEM_BYTES
            ),
            name="dispatch_up",
        )(x, expert, slot, gate, w_gate, w_up)

        tiles, ring = 8, 12
        width = d // tiles
        y = pl.pallas_call(
            functools.partial(second_kernel, (tiles, width, tokens, own, ring)),
            out_shape=jax.ShapeDtypeStruct((tokens, d), BF16),
            in_specs=[hbm] * 7,
            out_specs=hbm,
            scratch_shapes=[
                pltpu.VMEM((own, rows, ff), BF16),
                pltpu.VMEM((8, rows, tokens), BF16),
                pltpu.VMEM((tokens, d), BF16),
                pltpu.VMEM((tokens, 2 * ff), BF16),
                pltpu.VMEM((ring, ff, width), BF16),
                pltpu.VMEM((2, 2, d, width), BF16),
                pltpu.VMEM((2, 2 * ff, width), BF16),
                pltpu.VMEM((8, rows, width), BF16),
                pltpu.VMEM((tiles, 4, tokens, width), F32),
                pltpu.VMEM((3, 4, tokens, width), BF16),
                pltpu.VMEM((tiles, 4, tokens, width), BF16),
                pltpu.VMEM((tiles, 4, tokens // 2, width), BF16),
                pltpu.VMEM((tiles, 4, tokens // 2, width), BF16),
                pltpu.VMEM((tiles, 2, tokens // 2, width), BF16),
                pltpu.VMEM((tiles, 2, tokens // 2, width), BF16),
                pltpu.VMEM((2, tokens, width), BF16),
                dma((own + 2,)),
                dma((ring,)),
                dma((2, 2)),
                dma((2,)),
                dma((2,)),
                dma((tiles, 7)),
                dma((tiles, 7)),
            ],
            compiler_params=pltpu.CompilerParams(
                collective_id=1, has_side_effects=True, vmem_limit_bytes=VMEM_BYTES
            ),
            name="down_combine",
        )(h, ct, x, w_down, s_gate, s_up, s_down)
        return y[None, None]

    tok, exp, rep = P("dp", "ep"), P("ep"), P()
    return jax.shard_map(
        body,
        mesh=mesh,
        in_specs=(tok,) * 4 + (exp,) * 3 + (rep,) * 3,
        out_specs=tok,
        check_vma=False,
    )
```
